256 devices in a mesh: docs: 32 (over x, z), topics: 8 (over y, core).
Axes of the slice: x: 4, y: 4, z: 8, core: 2. Of those that a mesh axis runs over, the one named last changes fastest.
Arguments:
- log_beta: bfloat16 [262144, 2048], P('docs', 'topics'), may hold values from -250 to -4
- gamma_init: float32 [512, 2048], P('docs', 'topics'), may hold values from 0.05 to 5
- topic_prior: float32 [2048], P('topics'), may hold values from 0.02 to 0.5
- word_block: int32 [512, 256, 1], P('docs'), may hold values from 0 to 31; in each aligned block of 4096 rows (0 to 4095, 4096 to 8191, ..., all dimensions but the last counted through in order) at most 256 rows name the same one
- word_row: int32 [512, 256], P('docs'), may hold values from 0 to 8191
- counts: int32 [512, 256], P('docs'), may hold values from 0 to 2
Outputs:
- doc_gamma: float32 [512, 2048], P('docs', 'topics')
- sstats: float32 [262144, 2048], P('docs', 'topics')
The draws below stay inside these ranges and needn't reach their ends.
Inputs may be any that keep to these rules, and one draw needn't show every extreme that they name: `word_block`: among the token slots of one device's 16 documents, at most 256 name the same vocabulary block, and some block is named by exactly 256 of them on some device. `counts`: A count of 0 marks an empty slot.
All inputs are finite; a program needn't handle non-finite values.
Results may differ from the reference program's by a relative error of at most 0.0003.
Values may be sent and summed in bfloat16 or wider, within the bound.
A program may use at most 64 MiB of HBM per device.

```python
import math
import jax
import jax.numpy as jnp
import numpy as np
from jax import lax

K = 2048
VOCAB = 262144
LEN = 256
ITERS = 3
DOC_DEV = 16
DOCS = 512
VOC_DEV = 8192
CAP = 256
N_DOCS = 32


def draw_log_beta(key, part):
    values = jax.random.uniform(key, (VOCAB, K), jnp.float32, -14.0, -4.0)
    return values.astype(jnp.bfloat16)


def place_ends(result, key, least, largest):
    spot = [jax.random.randint(jax.random.fold_in(key, axis), (), 0, length) for axis, length in enumerate(result.shape)]
    widest = result.shape.index(max(result.shape))
    beside = spot[:widest] + [(spot[widest] + 1) % result.shape[widest]] + spot[widest + 1:]
    return result.at[tuple(spot)].set(least).at[tuple(beside)].set(largest)


def levels(key, extent, cuts, low, top_value):
    level, own = 1.0, jax.random.fold_in(key, 6)
    for dim, parts in cuts:
        heights = jnp.exp(jax.random.uniform(jax.random.fold_in(own, dim), (parts,), jnp.float32, low / len(cuts), top_value / len(cuts)))
        level = level * jnp.repeat(heights, extent[dim] // parts).reshape([-1 if axis == dim else 1 for axis in range(len(extent))])
    return level


def assign_block(rng, own, number, rows, count, top, bound, slope):
    order = jax.random.permutation(rng, count)
    packed, common = load_shares(count, rows * top, bound, slope, True), load_shares(count, rows * top, bound, slope, False)
    places = jnp.arange(count)

    def named(lengths, offset_by):
        used = int((lengths > 0).sum())
        fixed = max(1, used // 4)
        shifted = fixed + (places - fixed + offset_by * (used - fixed)) % max(1, count - fixed)
        return jnp.zeros((count,), jnp.int32).at[order[jnp.where(places < fixed, places, shifted)]].set(jnp.asarray(lengths, jnp.int32))

    lengths = jnp.where(number % 4 == 0, named(packed, number // 4), named(common, number - number // 4 - 1))
    mixed = jax.random.permutation(jax.random.fold_in(own, 3), count)
    source_of, receiver = mixed[0:count // 2 * 2:2], mixed[1:count // 2 * 2:2]
    room = jnp.minimum(lengths[source_of] - 1, bound - lengths[receiver]) // 2
    room = jnp.where((source_of == order[0]) | (receiver == order[0]) | (lengths[receiver] == 0), 0, jnp.maximum(room, 0))
    shifted = jax.random.randint(jax.random.fold_in(own, 4), (count // 2,), 0, 1 << 20) % (room + 1)
    lengths = lengths.at[source_of].add(-shifted).at[receiver].add(shifted)
    labels = jnp.searchsorted(jnp.cumsum(lengths), jnp.arange(rows * top), side="right").astype(jnp.int32)
    listing = labels.reshape(top, rows).T
    listing = listing[jax.random.permutation(jax.random.fold_in(own, 1), rows)]
    offset_by = jax.random.randint(jax.random.fold_in(own, 2), (rows, 1), 0, top)
    return jnp.take_along_axis(listing, (jnp.arange(top)[None, :] + offset_by) % top, axis=1)


def load_shares(number_of, total, bound, skew, full):
    weights = [(1 << 20) // math.isqrt(standing ** skew) + 1 for standing in range(1, number_of + 1)]
    largest = bound if full else min(bound, max(-(-total // number_of), total * weights[0] // sum(weights)))
    least = 1 if total - largest >= number_of - 1 else 0
    given, rest = [largest] + [least] * (number_of - 1), total - largest - least * (number_of - 1)
    while rest > 0:
        free = [i for i in range(1, number_of) if given[i] < largest] or [i for i in range(1, number_of) if given[i] < bound]
        pool, budget = sum([weights[i] for i in free]), rest
        for i in free:
            addition = min(bound - given[i], max(1, budget * weights[i] // pool), rest)
            given[i] = given[i] + addition
            rest = rest - addition
    return np.array(given)


def setup_inputs(seed: int = 0) -> dict:
    splits = jax.random.split(jax.random.key(seed), 7)
    log_beta = draw_log_beta(jax.random.fold_in(splits[6], 71), 0)
    gamma_init = jnp.clip(jnp.exp(math.log(5.0) - 4.6051702 * jax.random.uniform(splits[1], (DOCS, K), jnp.float32) ** levels(splits[1], (DOCS, K), ((0, 32), (1, 8)), -0.2, 0.2)), 0.05, 5.0)
    topic_prior = jnp.clip(jnp.exp(math.log(0.5) - 3.218876 * jax.random.uniform(splits[2], (K,), jnp.float32) ** levels(splits[2], (K,), ((0, 8),), -0.2, 0.2)), 0.02, 0.5)
    word_block_keys = jax.random.split(jax.random.fold_in(splits[3], 1), DOCS * LEN // (DOC_DEV * LEN))
    word_block_turns = jax.random.permutation(jax.random.fold_in(splits[3], 3), DOCS * LEN // (DOC_DEV * LEN))
    word_block = jax.vmap(lambda own, number: assign_block(jax.random.fold_in(splits[3], 2), own, number, DOC_DEV * LEN, N_DOCS, 1, CAP, 1))(word_block_keys, word_block_turns).reshape((DOCS, LEN, 1))
    word_row = place_ends(jax.random.randint(splits[4], (DOCS, LEN), 0, VOC_DEV), jax.random.fold_in(splits[4], 1), 0, VOC_DEV - 1).astype(jnp.int32)
    counts = place_ends(jax.random.randint(splits[5], (DOCS, LEN), 0, 3), jax.random.fold_in(splits[5], 1), 0, 2).astype(jnp.int32)
    return {"log_beta": log_beta, "gamma_init": gamma_init, "topic_prior": topic_prior, "word_block": word_block, "word_row": word_row, "counts": counts}


def expect_log(doc_gamma):
    return lax.digamma(doc_gamma)


def token_weights(log_theta, beta_rows):
    scores = log_theta[:, None, :] + beta_rows.astype(jnp.float32)
    row_max = jnp.max(scores, axis=2)
    exp_mass = jnp.sum(jnp.exp(scores - row_max[:, :, None]), axis=2)
    log_norm = row_max + jnp.log(exp_mass)
    return jnp.exp(scores - log_norm[:, :, None])


def reference(log_beta, gamma_init, topic_prior, word_block, word_row, counts):
    word_ids = word_block[:, :, 0] * VOC_DEV + word_row
    word_sets = word_ids.reshape(N_DOCS, DOC_DEV, LEN)
    count_sets = counts.astype(jnp.float32).reshape(N_DOCS, DOC_DEV, LEN)
    doc_gamma = gamma_init
    for sweep_index in range(ITERS):
        log_theta = expect_log(doc_gamma).reshape(N_DOCS, DOC_DEV, K)

        def renew_block(pieces):
            theta_part, word_part, count_part = pieces
            topic_share = token_weights(theta_part, log_beta[word_part])
            return topic_prior[None, :] + jnp.einsum("dn,dnk->dk", count_part, topic_share, precision=lax.Precision.HIGHEST)

        doc_gamma = lax.map(renew_block, (log_theta, word_sets, count_sets)).reshape(DOCS, K)
    final_theta = expect_log(doc_gamma).reshape(N_DOCS, DOC_DEV, K)

    def accumulate(doc_block, sstats):
        word_part = word_sets[doc_block]
        topic_share = token_weights(final_theta[doc_block], log_beta[word_part])
        contrib = count_sets[doc_block][:, :, None] * topic_share
        return sstats.at[word_part.reshape(-1)].add(contrib.reshape(-1, K))

    sstats = lax.fori_loop(0, N_DOCS, accumulate, jnp.zeros((VOCAB, K), jnp.float32))
    return doc_gamma, sstats
```

```python
import functools

import jax
import jax.numpy as jnp
from jax import lax
from jax.experimental import pallas as pl
from jax.experimental.pallas import tpu as pltpu
from jax.sharding import PartitionSpec as P

ITERS = 3
LIFT = 30.0
BF, F32, I32 = jnp.bfloat16, jnp.float32, jnp.int32
NT = (((1,), (1,)), ((), ()))


def dot(a, b, dims=(((1,), (0,)), ((), ()))):
    return lax.dot_general(a, b, dims, preferred_element_type=F32)


def halves(x):
    high = x.astype(BF)
    return high, (x - high.astype(F32)).astype(BF)


def iota(shape, dim):
    return lax.broadcasted_iota(I32, shape, dim)


def line(ref, at, first):
    return jnp.concatenate([ref[at, first : first + 1, :], ref[at, first + 1 : first + 2, :]], axis=1)


def pack_kernel(block_ref, row_ref, count_ref, out_ref):
    docs, length = block_ref.shape
    owners = out_ref.shape[0]
    cap = 256
    earlier = (iota((length, length), 0) < iota((length, length), 1)).astype(BF)

    def step(d, carry):
        total, offset = carry
        owner, row, count = (ref[pl.ds(d, 1), :] for ref in (block_ref, row_ref, count_ref))
        owner = jnp.where(count > 0, owner, -1)
        member = (iota((owners, length), 0) == owner).astype(F32)
        before = dot(member.astype(BF), earlier) + offset
        rank = jnp.sum(member * before, axis=0, keepdims=True).astype(I32)
        place = (iota((cap, length), 0) == rank).astype(BF)
        values = jnp.concatenate(
            [
                member * (row % 128).astype(F32),
                member * (row // 128).astype(F32),
                member * (count * docs + d).astype(F32),
            ],
            axis=0,
        ).astype(BF)
        total = total + dot(values, place, NT)
        return total, offset + jnp.sum(member, axis=1, keepdims=True)

    total, offset = lax.fori_loop(
        0, docs, step, (jnp.zeros((3 * owners, cap), F32), jnp.zeros((owners, 1), F32))
    )
    row = (total[owners : 2 * owners] * 128 + total[:owners]).astype(I32)
    rest = total[2 * owners :].astype(I32)
    used = jnp.broadcast_to(offset, (owners, 128)).astype(I32)
    for half in range(2):
        lanes = slice(half * 128, half * 128 + 128)
        out_ref[:, half, :] = row[:, lanes]
        out_ref[:, 2 + half, :] = rest[:, lanes] % docs
        out_ref[:, 4 + half, :] = rest[:, lanes] // docs
        out_ref[:, 6 + half, :] = used


def fetch_kernel(req_ref, beta_ref, high_ref, low_ref, shift_ref, wide, raw):
    owners = req_ref.shape[0]
    chunk = 256

    def widen(i, _):
        at = pl.ds(i * chunk, chunk)
        wide[at, :] = beta_ref[at, :].astype(F32)
        return 0

    lax.fori_loop(0, beta_ref.shape[0] // chunk, widen, 0)

    def one(s, _):
        raw[...] = jnp.zeros(raw.shape, F32)

        def eight(j, _):
            for u in range(8):
                n = j * 8 + u
                r = req_ref[s, n // 128, n % 128]
                raw[pl.ds(j * 8 + u, 1), :] = wide[pl.ds(r, 1), :]
            return 0

        lax.fori_loop(0, pl.cdiv(req_ref[s, 6, 0], 8), eight, 0)
        x = raw[...]
        shift = jnp.max(x, axis=1, keepdims=True) - LIFT
        high, low = halves(jnp.exp(x - shift))
        high_ref[pl.ds(s * chunk, chunk), :] = high
        low_ref[pl.ds(s * chunk, chunk), :] = low
        diagonal = iota((chunk, chunk), 0) == iota((chunk, chunk), 1)
        shift_ref[pl.ds(s, 1), :] = jnp.sum(jnp.where(diagonal, shift, 0.0), axis=0, keepdims=True)
        return 0

    lax.fori_loop(0, owners, one, 0)


def mass_kernel(docs, req_ref, theta_ref, high_ref, low_ref, out_ref):
    def one(s, _):
        high, low = halves(theta_ref[pl.ds(s * docs, docs), :])
        at = pl.ds(s * 256, 256)
        both = dot(jnp.concatenate([high, low], axis=0), high_ref[at, :], NT)
        mass = both[:docs] + both[docs:] + dot(high, low_ref[at, :], NT)
        mine = iota((docs, 256), 0) == line(req_ref, s, 2)
        out_ref[pl.ds(s, 1), :] = jnp.sum(jnp.where(mine, mass, 0.0), axis=0, keepdims=True)
        return 0

    lax.fori_loop(0, req_ref.shape[0], one, 0)


def slot_weights(me, docs, req_ref, shift_ref, mass_ref, s):
    shift = shift_ref[:, s, :]
    scale = jnp.exp(shift - jnp.max(shift, axis=0, keepdims=True))
    norm = jnp.sum(scale * mass_ref[:, s, :], axis=0, keepdims=True)
    own = jnp.sum(jnp.where(iota(scale.shape, 0) == me, scale, 0.0), axis=0, keepdims=True)
    weight = line(req_ref, s, 4).astype(F32) * own / norm
    return jnp.where(iota((docs, 256), 0) == line(req_ref, s, 2), weight, 0.0)


def gather_kernel(docs, req_ref, shift_ref, mass_ref, high_ref, low_ref, out_ref):
    me = lax.axis_index("topics")

    def one(s, _):
        high, low = halves(slot_weights(me, docs, req_ref, shift_ref, mass_ref, s))
        at = pl.ds(s * 256, 256)
        both = dot(jnp.concatenate([high, low], axis=0), high_ref[at, :])
        out_ref[pl.ds(s * docs, docs), :] = both[:docs] + both[docs:] + dot(high, low_ref[at, :])
        return 0

    lax.fori_loop(0, req_ref.shape[0], one, 0)


def stats_kernel(docs, req_ref, row_ref, theta_ref, shift_ref, mass_ref, high_ref, low_ref, out_ref, terms):
    me = lax.axis_index("topics")

    def clear(i, _):
        out_ref[pl.ds(i * 256, 256), :] = jnp.zeros((256, out_ref.shape[1]), F32)
        return 0

    lax.fori_loop(0, out_ref.shape[0] // 256, clear, 0)

    def one(s, _):
        whigh, wlow = halves(slot_weights(me, docs, req_ref, shift_ref, mass_ref, s))
        thigh, tlow = halves(theta_ref[pl.ds(s * docs, docs), :])
        at = pl.ds(s * 256, 256)
        share = lax.dot_general(
            jnp.concatenate([whigh, whigh, wlow], axis=0),
            jnp.concatenate([thigh, tlow, thigh], axis=0),
            (((0,), (0,)), ((), ())),
            preferred_element_type=F32,
        )
        terms[...] = share * (high_ref[at, :].astype(F32) + low_ref[at, :].astype(F32))

        def eight(j, _):
            for u in range(8):
                n = j * 8 + u
                r = pl.ds(row_ref[s, n // 128, n % 128], 1)
                out_ref[r, :] = out_ref[r, :] + terms[pl.ds(j * 8 + u, 1), :]
            return 0

        lax.fori_loop(0, pl.cdiv(row_ref[s, 6, 0], 8), eight, 0)
        return 0

    lax.fori_loop(0, req_ref.shape[0], one, 0)


VM = pl.BlockSpec(memory_space=pltpu.VMEM)
SM = pl.BlockSpec(memory_space=pltpu.SMEM)


def call(kernel, outs, specs, scratch=()):
    many = isinstance(outs, (list, tuple))
    return pl.pallas_call(
        kernel,
        out_shape=outs,
        in_specs=specs,
        out_specs=[VM] * len(outs) if many else VM,
        scratch_shapes=list(scratch),
        compiler_params=pltpu.CompilerParams(vmem_limit_bytes=56 * 2**20),
    )


def shape(s, t=F32):
    return jax.ShapeDtypeStruct(s, t)


def to_all(x, axis):
    n = lax.axis_size(axis)
    return lax.all_to_all(jnp.broadcast_to(x[None], (n, *x.shape)), axis, 0, 0, tiled=True)


def per_device(log_beta, gamma_init, topic_prior, word_block, word_row, counts):
    docs, length = counts.shape
    words, cols = log_beta.shape
    owners = lax.axis_size("docs")
    slots = owners * 256
    request = call(pack_kernel, shape((owners, 8, 128), I32), [VM] * 3)(
        word_block[:, :, 0], word_row, counts
    )
    req = lax.all_to_all(request, "docs", 0, 0, tiled=True)
    high, low, shift = call(
        fetch_kernel,
        [shape((slots, cols), BF), shape((slots, cols), BF), shape((owners, 256))],
        [SM, VM],
        [pltpu.VMEM((words, cols), F32), pltpu.VMEM((256, cols), F32)],
    )(req, log_beta)
    shifts = to_all(shift, "topics")
    gamma = gamma_init
    for sweep in range(ITERS + 1):
        theta = jnp.exp(lax.digamma(gamma))
        thetas = to_all(theta, "docs").reshape(owners * docs, cols)
        mass = call(functools.partial(mass_kernel, docs), shape((owners, 256)), [VM] * 4)(
            req, thetas, high, low
        )
        masses = to_all(mass, "topics")
        if sweep < ITERS:
            part = call(functools.partial(gather_kernel, docs), shape((owners * docs, cols)), [VM] * 5)(
                req, shifts, masses, high, low
            )
            parts = lax.all_to_all(part.reshape(owners, docs, cols), "docs", 0, 0, tiled=True)
            gamma = topic_prior[None, :] + theta * jnp.sum(parts, axis=0)
    stats = call(
        functools.partial(stats_kernel, docs),
        shape((words, cols)),
        [VM, SM] + [VM] * 5,
        [pltpu.VMEM((256, cols), F32)],
    )(req, req, thetas, shifts, masses, high, low)
    return gamma, stats


def solution(mesh):
    return jax.shard_map(
        per_device,
        mesh=mesh,
        in_specs=(
            P("docs", "topics"),
            P("docs", "topics"),
            P("topics"),
            P("docs", None, None),
            P("docs", None),
            P("docs", None),
        ),
        out_specs=(P("docs", "topics"), P("docs", "topics")),
        check_vma=False,
    )
```

```python
import functools

import jax
import jax.numpy as jnp
from jax import lax
from jax.experimental import pallas as pl
from jax.experimental.pallas import tpu as pltpu
from jax.sharding import PartitionSpec as P

ITERS = 3
LIFT = 30.0
BF, F32, I32 = jnp.bfloat16, jnp.float32, jnp.int32
NN = (((1,), (0,)), ((), ()))
NT = (((1,), (1,)), ((), ()))
TN = (((0,), (0,)), ((), ()))
MESH = pl.DeviceIdType.MESH
CAP = 256


def dot(a, b, dims=NN):
    return lax.dot_general(a, b, dims, preferred_element_type=F32)


def halves(x):
    high = x.astype(BF)
    return high, (x - high.astype(F32)).astype(BF)


def iota(shape, dim):
    return lax.broadcasted_iota(I32, shape, dim)


def grid_of(owners):
    return {32: 8}.get(owners, owners // 2)


def pack_kernel(block_ref, row_ref, count_ref, out_ref):
    docs, length = block_ref.shape
    owners = out_ref.shape[0]
    earlier = (iota((length, length), 0) < iota((length, length), 1)).astype(BF)

    def step(d, carry):
        total, offset = carry
        owner, row, count = (ref[pl.ds(d, 1), :] for ref in (block_ref, row_ref, count_ref))
        owner = jnp.where(count > 0, owner, -1)
        member = (iota((owners, length), 0) == owner).astype(F32)
        before = dot(member.astype(BF), earlier) + offset
        rank = jnp.sum(member * before, axis=0, keepdims=True).astype(I32)
        place = (iota((CAP, length), 0) == rank).astype(BF)
        values = jnp.concatenate(
            [
                member * (row % 128).astype(F32),
                member * (row // 128).astype(F32),
                member * (count * docs + d).astype(F32),
            ],
            axis=0,
        ).astype(BF)
        total = total + dot(values, place, NT)
        return total, offset + jnp.sum(member, axis=1, keepdims=True)

    total, offset = lax.fori_loop(
        0, docs, step, (jnp.zeros((3 * owners, CAP), F32), jnp.zeros((owners, 1), F32))
    )
    row = (total[owners : 2 * owners] * 128 + total[:owners]).astype(I32)
    rest = total[2 * owners :].astype(I32)
    used = jnp.broadcast_to(offset, (owners, 128)).astype(I32)
    for half in range(2):
        lanes = slice(half * 128, half * 128 + 128)
        out_ref[:, half, :] = row[:, lanes]
        out_ref[:, 2 + half, :] = rest[:, lanes] % docs
        out_ref[:, 4 + half, :] = rest[:, lanes] // docs
        out_ref[:, 6 + half, :] = used


def fetch_kernel(rows_ref, used_ref, beta_ref, high_ref, low_ref, shift_ref, wide, raw):
    owners = used_ref.shape[0]

    def widen(i, _):
        at = pl.ds(pl.multiple_of(i * CAP, CAP), CAP)
        wide[at, :] = beta_ref[at, :].astype(F32)
        return 0

    lax.fori_loop(0, beta_ref.shape[0] // CAP, widen, 0)
    raw[...] = jnp.zeros(raw.shape, F32)
    first = (iota((8, 128), 1) == 0).astype(BF)

    def one(s, _):
        def eight(j, _):
            to = raw.at[pl.ds(pl.multiple_of(j * 8, 8), 8), :]
            base = s * CAP + j * 8
            values = [wide[pl.ds(rows_ref[base + u], 1), :] for u in range(8)]
            for u in range(8):
                to[u : u + 1, :] = values[u]
            return 0

        lax.fori_loop(0, (used_ref[s] + 7) >> 3, eight, 0)
        x = raw[...]
        top = jnp.max(x, axis=1, keepdims=True)
        high, low = halves(jnp.exp(x - (top - LIFT)))
        at = pl.ds(pl.multiple_of(s * CAP, CAP), CAP)
        high_ref[at, :] = high
        low_ref[at, :] = low
        tops = dot(first, jnp.broadcast_to(top, (CAP, 128)).astype(BF), NT)
        shift_ref[pl.ds(s, 1), :] = tops[:1] - LIFT
        return 0

    lax.fori_loop(0, owners, one, 0)


def exp_digamma(g):
    z = g + 6.0
    total = 1.0 / g
    for i in range(1, 6):
        total = total + 1.0 / (g + float(i))
    inverse = 1.0 / z
    square = inverse * inverse
    series = square * (1 / 12 - square * (1 / 120 - square * (1 / 252 - square * (1 / 240))))
    return jnp.exp(jnp.log(z) - 0.5 * inverse - series - total)


def sweeps_kernel(
    nx, nz, groups,
    req_ref, gamma_ref, prior_ref, shift_ref, high_hbm, low_hbm,
    gamma_out, theta_out, weight_out,
    high_ref, low_ref, theta, own_theta, scales, masses, counts, holders, weights, parts, xparts, zbase, zparts,
    load_sem, shift_send, shift_recv, mass_send, mass_recv, tz_send, tz_recv, tx_send, tx_recv, sx_send, sx_recv, sz_send, sz_recv,
):
    owners = nx * nz
    docs = gamma_ref.shape[0]
    me, top = lax.axis_index("docs"), lax.axis_index("topics")
    x, z = me // nz, me % nz

    def at_x(d):
        return (x + d) % nx

    def at_z(d):
        return (z + d) % nz

    def block(i):
        return pl.ds(pl.multiple_of(i * docs, docs), docs)

    def remote(src, dst, send, recv, **device):
        return pltpu.make_async_remote_copy(
            src_ref=src, dst_ref=dst, send_sem=send, recv_sem=recv, device_id=device, device_id_type=MESH
        )

    barrier = pltpu.get_barrier_semaphore()
    for d in range(1, nz):
        pl.semaphore_signal(barrier, inc=1, device_id={"docs": x * nz + at_z(d)}, device_id_type=MESH)
    for d in range(1, nx):
        pl.semaphore_signal(barrier, inc=1, device_id={"docs": at_x(d) * nz + z}, device_id_type=MESH)
    for d in range(1, groups):
        pl.semaphore_signal(barrier, inc=1, device_id={"topics": (top + d) % groups}, device_id_type=MESH)
    loads = [
        pltpu.make_async_copy(high_hbm, high_ref, load_sem.at[0]),
        pltpu.make_async_copy(low_hbm, low_ref, load_sem.at[1]),
    ]
    for copy in loads:
        copy.start()
    counts[...] = jnp.concatenate([req_ref[:, 4, :], req_ref[:, 5, :]], axis=1).astype(F32)
    holders[...] = jnp.concatenate([req_ref[:, 2, :], req_ref[:, 3, :]], axis=1)
    gamma_out[...] = gamma_ref[...]
    first = exp_digamma(gamma_ref[...])
    own_theta[...] = first
    theta[block(me), :] = first
    scales[top] = shift_ref[...]
    pl.semaphore_wait(barrier, nz - 1 + nx - 1 + groups - 1)

    def shift_copy(d):
        return remote(shift_ref, scales.at[top], shift_send.at[d], shift_recv.at[d], topics=(top + d) % groups)

    for d in range(1, groups):
        shift_copy(d).start()

    def turn(k):
        return jnp.where(k % 2 == 1, (k + 1) // 2, (nz - k // 2) % nz)

    def tz_copy(d):
        return remote(theta.at[block(me)], theta.at[block(me)], tz_send.at[d], tz_recv.at[d], docs=x * nz + at_z(d))

    def tx_copy(dx, dz):
        b = block(x * nz + at_z(nz - dz))
        return remote(theta.at[b], theta.at[b], tx_send.at[dx, dz], tx_recv.at[dx, dz], docs=at_x(dx) * nz + z)

    def sx_copy(dx, dz):
        b = block(at_x(dx) * nz + at_z(dz))
        return remote(parts.at[b], xparts.at[dx, dz], sx_send.at[dx, dz], sx_recv.at[dx, dz], docs=at_x(dx) * nz + z)

    def sz_copy(d):
        return remote(zbase.at[d], zparts.at[d], sz_send.at[d], sz_recv.at[d], docs=x * nz + at_z(d))

    def mass_of(p, s):
        high, low = halves(theta[block(s), :])
        at = pl.ds(pl.multiple_of(s * CAP, CAP), CAP)
        both = dot(jnp.concatenate([high, low], axis=0), high_ref[at, :], NT)
        mass = both[:docs] + both[docs:] + dot(high, low_ref[at, :], NT)
        mine = iota((docs, CAP), 0) == holders[pl.ds(s, 1), :]
        masses[p, top, pl.ds(s, 1), :] = jnp.sum(jnp.where(mine, mass, 0.0), axis=0, keepdims=True)

    def masses_of(p, wait_loads):
        for d in range(1, nz):
            tz_copy(d).start()
        for d in range(1, nx):
            tx_copy(d, 0).start()
        if wait_loads:
            for copy in loads:
                copy.wait()
        mass_of(p, me)

        def column(k, _):
            dz = turn(k)
            tz_copy(dz).wait_recv()
            for d in range(1, nx):
                tx_copy(d, dz).start()
            mass_of(p, x * nz + at_z(nz - dz))
            return 0

        lax.fori_loop(1, nz, column, 0)

        def rest(k, _):
            dz = turn(k)
            for d in range(1, nx):
                tx_copy(d, dz).wait_recv()
            for d in range(1, nx):
                mass_of(p, at_x(nx - d) * nz + at_z(nz - dz))
            return 0

        lax.fori_loop(0, nz, rest, 0)

        def mass_copy(d):
            return remote(
                masses.at[p, top], masses.at[p, top], mass_send.at[d], mass_recv.at[p, d], topics=(top + d) % groups
            )

        for d in range(1, groups):
            mass_copy(d).start()
        for d in range(1, nz):
            tz_copy(d).wait_send()

        def sent(k, _):
            for d in range(1, nx):
                tx_copy(d, k).wait_send()
            return 0

        lax.fori_loop(0, nz, sent, 0)
        for d in range(1, groups):
            mass_copy(d).wait()
        if wait_loads:
            for d in range(1, groups):
                shift_copy(d).wait()
            peak = scales[0]
            for t in range(1, groups):
                peak = jnp.maximum(peak, scales[t])
            for t in range(groups):
                scales[t] = jnp.exp(scales[t] - peak)
        norm = scales[0] * masses[p, 0]
        for t in range(1, groups):
            norm = norm + scales[t] * masses[p, t]
        weights[...] = counts[...] * scales[top] / norm

    def part_of(s):
        mine = iota((docs, CAP), 0) == holders[pl.ds(s, 1), :]
        high, low = halves(jnp.where(mine, weights[pl.ds(s, 1), :], 0.0))
        at = pl.ds(pl.multiple_of(s * CAP, CAP), CAP)
        both = dot(jnp.concatenate([high, low], axis=0), high_ref[at, :])
        parts[block(s), :] = both[:docs] + both[docs:] + dot(high, low_ref[at, :])

    def renew():
        def scatter(k, _):
            dz = turn(nz - 1 - k)
            for d in range(nx):
                part_of(at_x(d) * nz + at_z(dz))
            for d in range(1, nx):
                sx_copy(d, dz).start()
            return 0

        lax.fori_loop(0, nz, scatter, 0)

        def joined(dz):
            total = parts[block(x * nz + at_z(dz)), :]
            for d in range(1, nx):
                sx_copy(d, dz).wait_recv()
                total = total + xparts[d, dz]
            return total

        def onward(k, _):
            dz = turn(nz - 1 - k)
            zbase[dz] = joined(dz)
            sz_copy(dz).start()
            return 0

        lax.fori_loop(0, nz - 1, onward, 0)
        total = joined(0)
        for d in range(1, nz):
            sz_copy(d).wait_recv()
            total = total + zparts[d]
        gamma = prior_ref[...] + own_theta[...] * total
        gamma_out[...] = gamma
        new = exp_digamma(gamma)
        own_theta[...] = new
        theta[block(me), :] = new
        for d in range(1, nz):
            sz_copy(d).wait_send()

        def sent(k, _):
            for d in range(1, nx):
                sx_copy(d, k).wait_send()
            return 0

        lax.fori_loop(0, nz, sent, 0)

    masses_of(0, True)
    renew()

    def sweep(i, _):
        masses_of(i % 2, False)
        renew()
        return 0

    lax.fori_loop(1, ITERS, sweep, 0)
    masses_of(ITERS % 2, False)
    weight_out[...] = weights[...]
    theta_out[...] = theta[...]


def stats_kernel(docs, rows_ref, used_ref, req_ref, theta_ref, weight_ref, high_ref, low_ref, out_ref, terms, *more):
    sums = (out_ref, *more)

    def clear(i, _):
        for total in sums:
            total[pl.ds(pl.multiple_of(i * CAP, CAP), CAP), :] = jnp.zeros((CAP, out_ref.shape[1]), F32)
        return 0

    lax.fori_loop(0, out_ref.shape[0] // CAP, clear, 0)

    def one(s, _):
        holder = jnp.concatenate([req_ref[s, 2:3, :], req_ref[s, 3:4, :]], axis=1)
        weight = jnp.where(iota((docs, CAP), 0) == holder, weight_ref[pl.ds(s, 1), :], 0.0)
        whigh, wlow = halves(weight)
        thigh, tlow = halves(theta_ref[pl.ds(pl.multiple_of(s * docs, docs), docs), :])
        at = pl.ds(pl.multiple_of(s * CAP, CAP), CAP)
        share = dot(
            jnp.concatenate([whigh, whigh, wlow], axis=0), jnp.concatenate([thigh, tlow, thigh], axis=0), TN
        )
        terms[...] = share * (high_ref[at, :].astype(F32) + low_ref[at, :].astype(F32))

        def eight(j, _):
            base = s * CAP + j * 8
            now = terms.at[pl.ds(pl.multiple_of(j * 8, 8), 8), :]
            rows = [rows_ref[base + u] for u in range(8)]
            for start in range(0, 8, len(sums)):
                news = []
                for k, total in enumerate(sums):
                    u = start + k
                    news.append(total[pl.ds(rows[u], 1), :] + now[u : u + 1, :])
                for k, total in enumerate(sums):
                    total[pl.ds(rows[start + k], 1), :] = news[k]
            return 0

        lax.fori_loop(0, (used_ref[s] + 7) >> 3, eight, 0)
        return 0

    lax.fori_loop(0, used_ref.shape[0], one, 0)

    def finish(i, _):
        at = pl.ds(pl.multiple_of(i * CAP, CAP), CAP)
        out_ref[at, :] = functools.reduce(jnp.add, [total[at, :] for total in sums])
        return 0

    lax.fori_loop(0, out_ref.shape[0] // CAP, finish, 0)


VM = pl.BlockSpec(memory_space=pltpu.VMEM)
SM = pl.BlockSpec(memory_space=pltpu.SMEM)
AN = pl.BlockSpec(memory_space=pl.ANY)


def call(kernel, outs, specs, scratch=(), **params):
    many = isinstance(outs, (list, tuple))
    return pl.pallas_call(
        kernel,
        out_shape=outs,
        in_specs=specs,
        out_specs=[VM] * len(outs) if many else VM,
        scratch_shapes=list(scratch),
        compiler_params=pltpu.CompilerParams(vmem_limit_bytes=60 * 2**20, **params),
    )


def shape(s, t=F32):
    return jax.ShapeDtypeStruct(s, t)


def per_device(log_beta, gamma_init, topic_prior, word_block, word_row, counts):
    docs, length = counts.shape
    words, cols = log_beta.shape
    owners, groups = lax.axis_size("docs"), lax.axis_size("topics")
    nz = grid_of(owners)
    nx = owners // nz
    slots = owners * CAP
    request = call(pack_kernel, shape((owners, 8, 128), I32), [VM] * 3)(
        word_block[:, :, 0], word_row, counts
    )
    req = lax.all_to_all(request, "docs", 0, 0, tiled=True)
    rows, used = req[:, :2, :].reshape(slots), req[:, 6, 0]
    high, low, shift = call(
        fetch_kernel,
        [shape((slots, cols), BF), shape((slots, cols), BF), shape((owners, CAP))],
        [SM, SM, VM],
        [pltpu.VMEM((words, cols), F32), pltpu.VMEM((CAP, cols), F32)],
    )(rows, used, log_beta)
    D = pltpu.SemaphoreType.DMA
    block = (docs, cols)
    gamma, theta, weight = call(
        functools.partial(sweeps_kernel, nx, nz, groups),
        [shape(block), shape((owners * docs, cols)), shape((owners, CAP))],
        [VM] * 4 + [AN] * 2,
        [
            pltpu.VMEM((slots, cols), BF),
            pltpu.VMEM((slots, cols), BF),
            pltpu.VMEM((owners * docs, cols), F32),
            pltpu.VMEM(block, F32),
            pltpu.VMEM((groups, owners, CAP), F32),
            pltpu.VMEM((2, groups, owners, CAP), F32),
            pltpu.VMEM((owners, CAP), F32),
            pltpu.VMEM((owners, CAP), I32),
            pltpu.VMEM((owners, CAP), F32),
            pltpu.VMEM((owners * docs, cols), F32),
            pltpu.VMEM((nx, nz, *block), F32),
            pltpu.VMEM((nz, *block), F32),
            pltpu.VMEM((nz, *block), F32),
            D((2,)), D((groups,)), D((groups,)), D((groups,)), D((2, groups)),
            D((nz,)), D((nz,)), D((nx, nz)), D((nx, nz)), D((nx, nz)), D((nx, nz)), D((nz,)), D((nz,)),
        ],
        collective_id=1,
        has_side_effects=True,
    )(req, gamma_init, topic_prior[None, :], shift, high, low)
    stats = call(
        functools.partial(stats_kernel, docs),
        shape((words, cols)),
        [SM, SM] + [VM] * 5,
        [pltpu.VMEM((CAP, cols), F32)] + [pltpu.VMEM((words, cols), F32)] * 3,
    )(rows, used, req, theta, weight, high, low)
    return gamma, stats


def solution(mesh):
    return jax.shard_map(
        per_device,
        mesh=mesh,
        in_specs=(
            P("docs", "topics"),
            P("docs", "topics"),
            P("topics"),
            P("docs", None, None),
            P("docs", None),
            P("docs", None),
        ),
        out_specs=(P("docs", "topics"), P("docs", "topics")),
        check_vma=False,
    )
```

```python
import functools

import jax
import jax.numpy as jnp
from jax import lax
from jax.experimental import pallas as pl
from jax.experimental.pallas import tpu as pltpu
from jax.sharding import PartitionSpec as P

ITERS = 3
LIFT = 30.0
BF, F32, I32 = jnp.bfloat16, jnp.float32, jnp.int32
NN = (((1,), (0,)), ((), ()))
NT = (((1,), (1,)), ((), ()))
TN = (((0,), (0,)), ((), ()))
MESH = pl.DeviceIdType.MESH
CAP = 256


def dot(a, b, dims=NN):
    return lax.dot_general(a, b, dims, preferred_element_type=F32)


def halves(x):
    high = x.astype(BF)
    return high, (x - high.astype(F32)).astype(BF)


def iota(shape, dim):
    return lax.broadcasted_iota(I32, shape, dim)


def grid_of(owners):
    return {32: 8}.get(owners, owners // 2)


def pack(words, block_ref, row_ref, count_ref, out_ref):
    docs, length = block_ref.shape
    owners = out_ref.shape[0]
    earlier = (iota((length, length), 0) < iota((length, length), 1)).astype(BF)

    def step(d, carry):
        total, offset = carry
        owner, row, count = (ref[pl.ds(d, 1), :] for ref in (block_ref, row_ref, count_ref))
        owner = jnp.where(count > 0, owner, -1)
        member = (iota((owners, length), 0) == owner).astype(F32)
        before = dot(member.astype(BF), earlier) + offset
        rank = jnp.sum(member * before, axis=0, keepdims=True).astype(I32)
        place = (iota((CAP, length), 0) == rank).astype(BF)
        values = jnp.concatenate(
            [
                member * (row % 128).astype(F32),
                member * (row // 128).astype(F32),
                member * (count * docs + d).astype(F32),
            ],
            axis=0,
        ).astype(BF)
        total = total + dot(values, place, NT)
        return total, offset + jnp.sum(member, axis=1, keepdims=True)

    total, offset = lax.fori_loop(
        0, docs, step, (jnp.zeros((3 * owners, CAP), F32), jnp.zeros((owners, 1), F32))
    )
    row = (total[owners : 2 * owners] * 128 + total[:owners]).astype(I32)
    row = jnp.minimum(jnp.maximum(row, 0), words - 1)
    rest = total[2 * owners :].astype(I32)
    used = jnp.broadcast_to(offset, (owners, 128)).astype(I32)
    for half in range(2):
        lanes = slice(half * 128, half * 128 + 128)
        out_ref[:, half, :] = row[:, lanes]
        out_ref[:, 2 + half, :] = rest[:, lanes] % docs
        out_ref[:, 4 + half, :] = rest[:, lanes] // docs
        out_ref[:, 6 + half, :] = used


def exp_digamma(g):
    z = g + 6.0
    total = 1.0 / g
    for i in range(1, 6):
        total = total + 1.0 / (g + float(i))
    inverse = 1.0 / z
    square = inverse * inverse
    series = square * (1 / 12 - square * (1 / 120 - square * (1 / 252 - square * (1 / 240))))
    return jnp.exp(jnp.log(z) - 0.5 * inverse - series - total)


def main_kernel(
    nx, nz, groups,
    block_ref, row_ref, count_ref, gamma_ref, prior_ref, beta_hbm,
    gamma_out, theta_out, weight_out, req, high_hbm, low_hbm,
    request, rows, beta, wide, raw, high_ref, low_ref, theta, own_theta,
    shifts, scales, masses, counts, holders, weights, parts, xparts, zbase, zparts,
    local_sem, rq_send, rq_recv, shift_send, shift_recv, mass_send, mass_recv,
    tz_send, tz_recv, tx_send, tx_recv, sx_send, sx_recv, sz_send, sz_recv,
):
    owners = nx * nz
    docs = gamma_ref.shape[0]
    me, top = lax.axis_index("docs"), lax.axis_index("topics")
    x, z = me // nz, me % nz
    chunks = nz // 2
    size = 2 * nx

    def at_x(d):
        return (x + d) % nx

    def at_z(d):
        return (z + d) % nz

    def block(i):
        return pl.ds(pl.multiple_of(i * docs, docs), docs)

    def slots(s):
        return pl.ds(pl.multiple_of(s * CAP, CAP), CAP)

    def lines(c):
        return pl.ds(pl.multiple_of(c * size, size), size)

    def remote(src, dst, send, recv, **device):
        return pltpu.make_async_remote_copy(
            src_ref=src, dst_ref=dst, send_sem=send, recv_sem=recv, device_id=device, device_id_type=MESH
        )

    def each(n, body, first=1):
        lax.fori_loop(first, n, lambda i, _: (body(i), 0)[1], 0)

    barrier = pltpu.get_barrier_semaphore()
    each(
        owners,
        lambda d: pl.semaphore_signal(
            barrier, inc=1, device_id={"docs": (me + d) % owners}, device_id_type=MESH
        ),
    )
    for d in range(1, groups):
        pl.semaphore_signal(barrier, inc=1, device_id={"topics": (top + d) % groups}, device_id_type=MESH)
    load = pltpu.make_async_copy(beta_hbm, beta, local_sem.at[0])
    load.start()
    pack(beta.shape[0], block_ref, row_ref, count_ref, request)
    first = exp_digamma(gamma_ref[...])
    own_theta[...] = first
    theta[block(me), :] = first
    req[me] = request[me]
    pl.semaphore_wait(barrier, owners - 1 + groups - 1)

    def turn(k):
        return jnp.where(k % 2 == 1, (k + 1) // 2, (nz - k // 2) % nz)

    def rq_copy(d):
        to = (me + d) % owners
        return remote(request.at[to], req.at[me], rq_send.at[d], rq_recv.at[d], docs=to)

    def tz_copy(d):
        return remote(theta.at[block(me)], theta.at[block(me)], tz_send.at[d], tz_recv.at[d], docs=x * nz + at_z(d))

    def tx_copy(dx, dz):
        b = block(x * nz + at_z(nz - dz))
        return remote(theta.at[b], theta.at[b], tx_send.at[dx, dz], tx_recv.at[dx, dz], docs=at_x(dx) * nz + z)

    def sx_copy(dx, dz):
        b = block(at_x(dx) * nz + at_z(dz))
        return remote(parts.at[b], xparts.at[dx, dz], sx_send.at[dx, dz], sx_recv.at[dx, dz], docs=at_x(dx) * nz + z)

    def sz_copy(d):
        return remote(zbase.at[d], zparts.at[d], sz_send.at[d], sz_recv.at[d], docs=x * nz + at_z(d))

    def shift_copy(d, c):
        a = shifts.at[top, lines(c)]
        return remote(a, a, shift_send.at[d, c], shift_recv.at[d, c], topics=(top + d) % groups)

    def mass_copy(p, d, c):
        a = masses.at[p, top, lines(c)]
        return remote(a, a, mass_send.at[d, c], mass_recv.at[p, d, c], topics=(top + d) % groups)

    def source(k, d):
        return at_x(nx - d) * nz + at_z(nz - turn(k))

    def send_theta():
        each(nz, lambda d: tz_copy(d).start())
        for d in range(1, nx):
            tx_copy(d, 0).start()

    def forward(k):
        dz = turn(k)
        tz_copy(dz).wait_recv()
        for d in range(1, nx):
            tx_copy(d, dz).start()

    def mass_of(p, k, d):
        s, q = source(k, d), k * nx + d
        high, low = halves(theta[block(s), :])
        both = dot(jnp.concatenate([high, low], axis=0), high_ref[slots(s), :], NT)
        mass = both[:docs] + both[docs:] + dot(high, low_ref[slots(s), :], NT)
        mine = iota((docs, CAP), 0) == holders[pl.ds(q, 1), :]
        masses[p, top, pl.ds(q, 1), :] = jnp.sum(jnp.where(mine, mass, 0.0), axis=0, keepdims=True)

    def masses_of(p, c):
        def two(k):
            for d in range(1, nx):
                tx_copy(d, turn(k)).wait_recv()
            for d in range(nx):
                mass_of(p, k, d)

        each(2 * c + 2, two, 2 * c)
        each(groups, lambda d: mass_copy(p, d, c).start())

    def sent_theta():
        each(nz, lambda d: tz_copy(d).wait_send())

        def sent(k):
            for d in range(1, nx):
                tx_copy(d, k).wait_send()

        each(nz, sent, 0)

    send_theta()
    each(owners, lambda d: rq_copy(d).start())
    load.wait()

    def widen(i):
        wide[slots(i), :] = beta[slots(i), :].astype(F32)

    each(beta.shape[0] // CAP, widen, 0)
    each(nz, forward)
    each(owners, lambda d: rq_copy(d).wait_recv())
    to_scalars = pltpu.make_async_copy(req.at[:, 0:2, :], rows, local_sem.at[0])
    to_scalars.start()

    def arrange(k):
        for d in range(nx):
            s, q = source(k, d), k * nx + d
            holders[pl.ds(q, 1), :] = jnp.concatenate([req[s, 2:3, :], req[s, 3:4, :]], axis=1)
            counts[pl.ds(q, 1), :] = jnp.concatenate([req[s, 4:5, :], req[s, 5:6, :]], axis=1).astype(F32)

    each(nz, arrange, 0)
    to_scalars.wait()
    lead = (iota((8, 128), 1) == 0).astype(BF)

    def fetch(q):
        s = source(q // nx, q % nx)
        for start in range(0, CAP, 16):
            values = [wide[pl.ds(rows[s, n // 128, n % 128], 1), :] for n in range(start, start + 16)]
            for u in range(16):
                raw[start + u : start + u + 1, :] = values[u]
        value = raw[...]
        peak = jnp.max(value, axis=1, keepdims=True)
        high, low = halves(jnp.exp(value - (peak - LIFT)))
        high_ref[slots(s), :] = high
        low_ref[slots(s), :] = low
        peaks = dot(lead, jnp.broadcast_to(peak, (CAP, 128)).astype(BF), NT)
        shifts[top, pl.ds(q, 1), :] = peaks[:1] - LIFT

    def begin(c):
        each(size * (c + 1), fetch, size * c)
        each(groups, lambda d: shift_copy(d, c).start())
        masses_of(0, c)

    each(chunks, begin, 0)
    keeps = [
        pltpu.make_async_copy(high_ref, high_hbm, local_sem.at[0]),
        pltpu.make_async_copy(low_ref, low_hbm, local_sem.at[1]),
    ]
    for copy in keeps:
        copy.start()
    sent_theta()
    each(owners, lambda d: rq_copy(d).wait_send())

    def scale(c):
        each(groups, lambda d: shift_copy(d, c).wait())
        peak = shifts[0, lines(c), :]
        for t in range(1, groups):
            peak = jnp.maximum(peak, shifts[t, lines(c), :])
        for t in range(groups):
            scales[t, lines(c), :] = jnp.exp(shifts[t, lines(c), :] - peak)

    def weigh(p, c):
        each(groups, lambda d: mass_copy(p, d, c).wait())
        norm = scales[0, lines(c), :] * masses[p, 0, lines(c), :]
        for t in range(1, groups):
            norm = norm + scales[t, lines(c), :] * masses[p, t, lines(c), :]
        weights[lines(c), :] = counts[lines(c), :] * scales[top, lines(c), :] / norm

    def part_of(k, d):
        s, q = source(k, d), k * nx + d
        mine = iota((docs, CAP), 0) == holders[pl.ds(q, 1), :]
        high, low = halves(jnp.where(mine, weights[pl.ds(q, 1), :], 0.0))
        both = dot(jnp.concatenate([high, low], axis=0), high_ref[slots(s), :])
        parts[block(s), :] = both[:docs] + both[docs:] + dot(high, low_ref[slots(s), :])

    def back(k):
        return (nz - turn(k)) % nz

    def parts_of(c):
        def two(k):
            for d in range(nx):
                part_of(k, d)
            for d in range(1, nx):
                sx_copy(d, back(k)).start()

        each(2 * c + 2, two, 2 * c)

    def joined(dz):
        total = parts[block(x * nz + at_z(dz)), :]
        for d in range(1, nx):
            sx_copy(d, dz).wait_recv()
            total = total + xparts[d, dz]
        return total

    def onward(k):
        zbase[back(k)] = joined(back(k))
        sz_copy(back(k)).start()

    def renew(p, prepare):
        def share(c):
            prepare(c)
            weigh(p, c)
            parts_of(c)

        each(chunks, share, 0)
        each(nz, onward)
        total = joined(0)
        for d in range(1, nz):
            sz_copy(d).wait_recv()
            total = total + zparts[d]
        gamma = prior_ref[...] + own_theta[...] * total
        gamma_out[...] = gamma
        new = exp_digamma(gamma)
        own_theta[...] = new
        theta[block(me), :] = new
        send_theta()
        each(nz, lambda d: sz_copy(d).wait_send())

        def sent(k):
            for d in range(1, nx):
                sx_copy(d, k).wait_send()

        each(nz, sent, 0)

    def collect(p):
        each(2, forward)
        each(
            chunks,
            lambda c: (each(jnp.minimum(2 * c + 4, nz), forward, 2 * c + 2), masses_of(p, c)),
            0,
        )
        sent_theta()

    renew(0, scale)

    def sweep(i):
        collect(i % 2)
        renew(i % 2, lambda c: None)

    each(ITERS, sweep)
    collect(ITERS % 2)
    each(chunks, lambda c: weigh(ITERS % 2, c), 0)

    def deliver(k):
        for d in range(nx):
            weight_out[pl.ds(source(k, d), 1), :] = weights[pl.ds(k * nx + d, 1), :]

    each(nz, deliver, 0)
    theta_out[...] = theta[...]
    for copy in keeps:
        copy.wait()


def stats_kernel(docs, rows_ref, used_ref, req_ref, theta_ref, weight_ref, high_hbm, low_hbm, out_hbm, terms, high_ref, low_ref, sem, *sums):
    loads = [
        pltpu.make_async_copy(high_hbm, high_ref, sem.at[0]),
        pltpu.make_async_copy(low_hbm, low_ref, sem.at[1]),
    ]
    for copy in loads:
        copy.start()

    def clear(i, _):
        for total in sums:
            total[pl.ds(pl.multiple_of(i * CAP, CAP), CAP), :] = jnp.zeros((CAP, out_hbm.shape[1]), F32)
        return 0

    lax.fori_loop(0, out_hbm.shape[0] // CAP, clear, 0)
    for copy in loads:
        copy.wait()

    def one(s, _):
        holder = jnp.concatenate([req_ref[s, 2:3, :], req_ref[s, 3:4, :]], axis=1)
        weight = jnp.where(iota((docs, CAP), 0) == holder, weight_ref[pl.ds(s, 1), :], 0.0)
        whigh, wlow = halves(weight)
        thigh, tlow = halves(theta_ref[pl.ds(pl.multiple_of(s * docs, docs), docs), :])
        at = pl.ds(pl.multiple_of(s * CAP, CAP), CAP)
        share = dot(
            jnp.concatenate([whigh, whigh, wlow], axis=0), jnp.concatenate([thigh, tlow, thigh], axis=0), TN
        )
        terms[...] = share * (high_ref[at, :].astype(F32) + low_ref[at, :].astype(F32))

        def eight(j, _):
            base = s * CAP + j * 8
            now = terms.at[pl.ds(pl.multiple_of(j * 8, 8), 8), :]
            rows = [rows_ref[base + u] for u in range(8)]
            for start in range(0, 8, len(sums)):
                news = []
                for k, total in enumerate(sums):
                    u = start + k
                    news.append(total[pl.ds(rows[u], 1), :] + now[u : u + 1, :])
                for k, total in enumerate(sums):
                    total[pl.ds(rows[start + k], 1), :] = news[k]
            return 0

        lax.fori_loop(0, (used_ref[s] + 7) >> 3, eight, 0)
        return 0

    lax.fori_loop(0, used_ref.shape[0], one, 0)

    def finish(i, _):
        at = pl.ds(pl.multiple_of(i * CAP, CAP), CAP)
        sums[0][at, :] = functools.reduce(jnp.add, [total[at, :] for total in sums])
        pltpu.make_async_copy(sums[0].at[at], out_hbm.at[at], sem.at[2]).start()
        return 0

    lax.fori_loop(0, out_hbm.shape[0] // CAP, finish, 0)
    pltpu.make_async_copy(sums[0], out_hbm, sem.at[2]).wait()


VM = pl.BlockSpec(memory_space=pltpu.VMEM)
SM = pl.BlockSpec(memory_space=pltpu.SMEM)
AN = pl.BlockSpec(memory_space=pl.ANY)


def call(kernel, outs, in_specs, out_specs, scratch, **params):
    return pl.pallas_call(
        kernel,
        out_shape=outs,
        in_specs=in_specs,
        out_specs=out_specs,
        scratch_shapes=list(scratch),
        compiler_params=pltpu.CompilerParams(vmem_limit_bytes=60 * 2**20, **params),
    )


def shape(s, t=F32):
    return jax.ShapeDtypeStruct(s, t)


def per_device(log_beta, gamma_init, topic_prior, word_block, word_row, counts):
    docs, length = counts.shape
    words, cols = log_beta.shape
    owners, groups = lax.axis_size("docs"), lax.axis_size("topics")
    nz = grid_of(owners)
    nx = owners // nz
    slots = owners * CAP
    D, V = pltpu.SemaphoreType.DMA, pltpu.VMEM
    block = (docs, cols)
    gamma, theta, weight, req, high, low = call(
        functools.partial(main_kernel, nx, nz, groups),
        [
            shape(block), shape((owners * docs, cols)), shape((owners, CAP)), shape((owners, 8, 128), I32),
            shape((slots, cols), BF), shape((slots, cols), BF),
        ],
        [VM] * 5 + [AN],
        [VM] * 4 + [AN] * 2,
        [
            V((owners, 8, 128), I32),
            pltpu.SMEM((owners, 2, 128), I32),
            V((words, cols), BF),
            V((words, cols), F32),
            V((CAP, cols), F32),
            V((slots, cols), BF),
            V((slots, cols), BF),
            V((owners * docs, cols), F32),
            V(block, F32),
            V((groups, owners, CAP), F32),
            V((groups, owners, CAP), F32),
            V((2, groups, owners, CAP), F32),
            V((owners, CAP), F32),
            V((owners, CAP), I32),
            V((owners, CAP), F32),
            V((owners * docs, cols), F32),
            V((nx, nz, *block), F32),
            V((nz, *block), F32),
            V((nz, *block), F32),
            D((2,)), D((owners,)), D((owners,)), D((groups, nz // 2)), D((groups, nz // 2)),
            D((groups, nz // 2)), D((2, groups, nz // 2)),
            D((nz,)), D((nz,)), D((nx, nz)), D((nx, nz)), D((nx, nz)), D((nx, nz)), D((nz,)), D((nz,)),
        ],
        collective_id=1,
        has_side_effects=True,
    )(word_block[:, :, 0], word_row, counts, gamma_init, topic_prior[None, :], log_beta)
    rows, used = req[:, :2, :].reshape(slots), req[:, 6, 0]
    stats = call(
        functools.partial(stats_kernel, docs),
        shape((words, cols)),
        [SM, SM] + [VM] * 3 + [AN] * 2,
        AN,
        [V((CAP, cols), F32), V((slots, cols), BF), V((slots, cols), BF), D((3,))]
        + [V((words, cols), F32)] * 4,
    )(rows, used, req, theta, weight, high, low)
    return gamma, stats


def solution(mesh):
    return jax.shard_map(
        per_device,
        mesh=mesh,
        in_specs=(
            P("docs", "topics"),
            P("docs", "topics"),
            P("topics"),
            P("docs", None, None),
            P("docs", None),
            P("docs", None),
        ),
        out_specs=(P("docs", "topics"), P("docs", "topics")),
        check_vma=False,
    )
```

```python
import functools

import jax
import jax.numpy as jnp
from jax import lax
from jax.experimental import pallas as pl
from jax.experimental.pallas import tpu as pltpu
from jax.sharding import PartitionSpec as P

ITERS = 3
LIFT = 30.0
BF, F32, I32 = jnp.bfloat16, jnp.float32, jnp.int32
NN = (((1,), (0,)), ((), ()))
NT = (((1,), (1,)), ((), ()))
TN = (((0,), (0,)), ((), ()))
MESH = pl.DeviceIdType.MESH
CAP = 256


def dot(a, b, dims=NN):
    return lax.dot_general(a, b, dims, preferred_element_type=F32)


def halves(x):
    high = x.astype(BF)
    return high, (x - high.astype(F32)).astype(BF)


def iota(shape, dim):
    return lax.broadcasted_iota(I32, shape, dim)


def grid_of(owners):
    return {32: 8}.get(owners, owners // 2)


def pack(words, block_ref, row_ref, count_ref, out_ref):
    docs, length = row_ref.shape
    owners = out_ref.shape[0]
    earlier = (iota((length, length), 0) < iota((length, length), 1)).astype(BF)

    def step(d, carry):
        total, offset = carry
        owner, row, count = block_ref[d], row_ref[pl.ds(d, 1), :], count_ref[pl.ds(d, 1), :]
        owner = jnp.where(count > 0, owner, -1)
        member = (iota((owners, length), 0) == owner).astype(F32)
        before = dot(member.astype(BF), earlier) + offset
        rank = jnp.sum(member * before, axis=0, keepdims=True).astype(I32)
        place = (iota((CAP, length), 0) == rank).astype(BF)
        values = jnp.concatenate(
            [
                member * (row % 128).astype(F32),
                member * (row // 128).astype(F32),
                member * (count * docs + d).astype(F32),
            ],
            axis=0,
        ).astype(BF)
        total = total + dot(values, place, NT)
        return total, offset + jnp.sum(member, axis=1, keepdims=True)

    together = 4 if docs % 4 == 0 else 1

    def steps(i, carry):
        for u in range(together):
            carry = step(i * together + u, carry)
        return carry

    total, offset = lax.fori_loop(
        0, docs // together, steps, (jnp.zeros((3 * owners, CAP), F32), jnp.zeros((owners, 1), F32))
    )
    row = (total[owners : 2 * owners] * 128 + total[:owners]).astype(I32)
    row = jnp.minimum(jnp.maximum(row, 0), words - 1)
    rest = total[2 * owners :].astype(I32)
    used = jnp.broadcast_to(offset, (owners, 128)).astype(I32)
    for half in range(2):
        lanes = slice(half * 128, half * 128 + 128)
        out_ref[:, half, :] = row[:, lanes]
        out_ref[:, 2 + half, :] = rest[:, lanes] % docs
        out_ref[:, 4 + half, :] = rest[:, lanes] // docs
        out_ref[:, 6 + half, :] = used


def exp_digamma(g):
    z = g + 6.0
    total = 1.0 / g
    for i in range(1, 6):
        total = total + 1.0 / (g + float(i))
    inverse = 1.0 / z
    square = inverse * inverse
    series = square * (1 / 12 - square * (1 / 120 - square * (1 / 252 - square * (1 / 240))))
    return jnp.exp(jnp.log(z) - 0.5 * inverse - series - total)


def main_kernel(
    nx, nz, groups,
    block_ref, row_ref, count_ref, gamma_ref, prior_ref, beta_hbm,
    gamma_out, theta_out, weight_out, holder_out, row_out, used_out, high_hbm, low_hbm,
    request, req, rows, beta, wide, raw, high_ref, low_ref, theta, own_theta,
    shifts, scales, masses, counts, holders, weights, parts, xparts, zbase, zparts,
    local_sem, rq_send, rq_recv, shift_send, shift_recv, mass_send, mass_recv,
    tz_send, tz_recv, tx_send, tx_recv, sx_send, sx_recv, sz_send, sz_recv,
):
    owners = nx * nz
    docs = gamma_ref.shape[0]
    me, top = lax.axis_index("docs"), lax.axis_index("topics")
    x, z = me // nz, me % nz
    chunks = nz // 2
    size = 2 * nx

    def at_x(d):
        return (x + d) % nx

    def at_z(d):
        return (z + d) % nz

    def block(i):
        return pl.ds(pl.multiple_of(i * docs, docs), docs)

    def slots(s):
        return pl.ds(pl.multiple_of(s * CAP, CAP), CAP)

    def lines(c):
        return pl.ds(pl.multiple_of(c * size, size), size)

    def remote(src, dst, send, recv, **device):
        return pltpu.make_async_remote_copy(
            src_ref=src, dst_ref=dst, send_sem=send, recv_sem=recv, device_id=device, device_id_type=MESH
        )

    def each(n, body, first=1):
        lax.fori_loop(first, n, lambda i, _: (body(i), 0)[1], 0)

    barrier = pltpu.get_barrier_semaphore()
    each(
        owners,
        lambda d: pl.semaphore_signal(
            barrier, inc=1, device_id={"docs": (me + d) % owners}, device_id_type=MESH
        ),
    )
    for d in range(1, groups):
        pl.semaphore_signal(barrier, inc=1, device_id={"topics": (top + d) % groups}, device_id_type=MESH)
    load = pltpu.make_async_copy(beta_hbm, beta, local_sem.at[0])
    load.start()
    pack(beta.shape[0], block_ref, row_ref, count_ref, request)
    first = exp_digamma(gamma_ref[...])
    own_theta[...] = first
    theta[block(me), :] = first
    req[me] = request[me]
    pl.semaphore_wait(barrier, owners - 1 + groups - 1)

    def turn(k):
        return jnp.where(k % 2 == 1, (k + 1) // 2, (nz - k // 2) % nz)

    def rq_copy(d):
        to = (me + d) % owners
        return remote(request.at[to], req.at[me], rq_send.at[d], rq_recv.at[d], docs=to)

    def tz_copy(d):
        return remote(theta.at[block(me)], theta.at[block(me)], tz_send.at[d], tz_recv.at[d], docs=x * nz + at_z(d))

    def tx_copy(dx, dz):
        b = block(x * nz + at_z(nz - dz))
        return remote(theta.at[b], theta.at[b], tx_send.at[dx, dz], tx_recv.at[dx, dz], docs=at_x(dx) * nz + z)

    def sx_copy(dx, dz):
        b = block(at_x(dx) * nz + at_z(dz))
        return remote(parts.at[b], xparts.at[dx, dz], sx_send.at[dx, dz], sx_recv.at[dx, dz], docs=at_x(dx) * nz + z)

    def sz_copy(d):
        return remote(zbase.at[d], zparts.at[d], sz_send.at[d], sz_recv.at[d], docs=x * nz + at_z(d))

    def shift_copy(d, c):
        a = shifts.at[top, lines(c)]
        return remote(a, a, shift_send.at[d, c], shift_recv.at[d, c], topics=(top + d) % groups)

    def mass_copy(p, d, c):
        a = masses.at[p, top, lines(c)]
        return remote(a, a, mass_send.at[d, c], mass_recv.at[p, d, c], topics=(top + d) % groups)

    def source(k, d):
        return at_x(nx - d) * nz + at_z(nz - turn(k))

    def send_theta():
        each(nz, lambda d: tz_copy(d).start())
        for d in range(1, nx):
            tx_copy(d, 0).start()

    def forward(k):
        dz = turn(k)
        tz_copy(dz).wait_recv()
        for d in range(1, nx):
            tx_copy(d, dz).start()

    def mass_of(p, k, d):
        s, q = source(k, d), k * nx + d
        high, low = halves(theta[block(s), :])
        both = dot(jnp.concatenate([high, low], axis=0), high_ref[slots(s), :], NT)
        mass = both[:docs] + both[docs:] + dot(high, low_ref[slots(s), :], NT)
        mine = iota((docs, CAP), 0) == holders[pl.ds(q, 1), :]
        masses[p, top, pl.ds(q, 1), :] = jnp.sum(jnp.where(mine, mass, 0.0), axis=0, keepdims=True)

    def masses_of(p, c):
        def two(k):
            for d in range(1, nx):
                tx_copy(d, turn(k)).wait_recv()
            for d in range(nx):
                mass_of(p, k, d)

        each(2 * c + 2, two, 2 * c)
        each(groups, lambda d: mass_copy(p, d, c).start())

    def sent_theta():
        each(nz, lambda d: tz_copy(d).wait_send())

        def sent(k):
            for d in range(1, nx):
                tx_copy(d, k).wait_send()

        each(nz, sent, 0)

    send_theta()
    each(owners, lambda d: rq_copy(d).start())
    load.wait()

    def widen(i):
        wide[slots(i), 0, :] = beta[slots(i), :].astype(F32)

    each(beta.shape[0] // CAP, widen, 0)
    each(nz, forward)
    each(owners, lambda d: rq_copy(d).wait_recv())
    to_scalars = pltpu.make_async_copy(req.at[:, 0:2, :], rows, local_sem.at[0])
    to_scalars.start()

    def arrange(k):
        for d in range(nx):
            s, q = source(k, d), k * nx + d
            holders[pl.ds(q, 1), :] = jnp.concatenate([req[s, 2:3, :], req[s, 3:4, :]], axis=1)
            counts[pl.ds(q, 1), :] = jnp.concatenate([req[s, 4:5, :], req[s, 5:6, :]], axis=1).astype(F32)

    each(nz, arrange, 0)
    to_scalars.wait()
    lead = (iota((8, 128), 1) == 0).astype(BF)

    def fetch(q):
        s = source(q // nx, q % nx)
        for start in range(0, CAP, 16):
            values = [wide[rows[s, n // 128, n % 128]] for n in range(start, start + 16)]
            for u in range(16):
                raw[start + u : start + u + 1, :] = values[u]
        value = raw[...]
        peak = jnp.max(value, axis=1, keepdims=True)
        high, low = halves(jnp.exp(value - (peak - LIFT)))
        high_ref[slots(s), :] = high
        low_ref[slots(s), :] = low
        peaks = dot(lead, jnp.broadcast_to(peak, (CAP, 128)).astype(BF), NT)
        shifts[top, pl.ds(q, 1), :] = peaks[:1] - LIFT

    def begin(c):
        each(size * (c + 1), fetch, size * c)
        each(groups, lambda d: shift_copy(d, c).start())
        masses_of(0, c)

    each(chunks, begin, 0)
    keeps = [
        pltpu.make_async_copy(high_ref, high_hbm, local_sem.at[0]),
        pltpu.make_async_copy(low_ref, low_hbm, local_sem.at[1]),
    ]
    for copy in keeps:
        copy.start()
    sent_theta()
    each(owners, lambda d: rq_copy(d).wait_send())

    def scale(c):
        each(groups, lambda d: shift_copy(d, c).wait())
        peak = shifts[0, lines(c), :]
        for t in range(1, groups):
            peak = jnp.maximum(peak, shifts[t, lines(c), :])
        for t in range(groups):
            scales[t, lines(c), :] = jnp.exp(shifts[t, lines(c), :] - peak)

    def weigh(p, c):
        each(groups, lambda d: mass_copy(p, d, c).wait())
        norm = scales[0, lines(c), :] * masses[p, 0, lines(c), :]
        for t in range(1, groups):
            norm = norm + scales[t, lines(c), :] * masses[p, t, lines(c), :]
        weights[lines(c), :] = counts[lines(c), :] * scales[top, lines(c), :] / norm

    def part_of(k, d):
        s, q = source(k, d), k * nx + d
        mine = iota((docs, CAP), 0) == holders[pl.ds(q, 1), :]
        high, low = halves(jnp.where(mine, weights[pl.ds(q, 1), :], 0.0))
        both = dot(jnp.concatenate([high, low], axis=0), high_ref[slots(s), :])
        parts[block(s), :] = both[:docs] + both[docs:] + dot(high, low_ref[slots(s), :])

    def back(k):
        return (nz - turn(k)) % nz

    def parts_of(c):
        def two(k):
            for d in range(nx):
                part_of(k, d)
            for d in range(1, nx):
                sx_copy(d, back(k)).start()

        each(2 * c + 2, two, 2 * c)

    def joined(dz):
        total = parts[block(x * nz + at_z(dz)), :]
        for d in range(1, nx):
            sx_copy(d, dz).wait_recv()
            total = total + xparts[d, dz]
        return total

    def onward(k):
        zbase[back(k)] = joined(back(k))
        sz_copy(back(k)).start()

    def renew(p, prepare):
        def share(c):
            prepare(c)
            weigh(p, c)
            parts_of(c)

        each(chunks, share, 0)
        each(nz, onward)
        total = joined(0)
        for d in range(1, nz):
            sz_copy(d).wait_recv()
            total = total + zparts[d]
        gamma = prior_ref[...] + own_theta[...] * total
        gamma_out[...] = gamma
        new = exp_digamma(gamma)
        own_theta[...] = new
        theta[block(me), :] = new
        send_theta()
        each(nz, lambda d: sz_copy(d).wait_send())

        def sent(k):
            for d in range(1, nx):
                sx_copy(d, k).wait_send()

        each(nz, sent, 0)

    def collect(p):
        each(2, forward)
        each(
            chunks,
            lambda c: (each(jnp.minimum(2 * c + 4, nz), forward, 2 * c + 2), masses_of(p, c)),
            0,
        )
        sent_theta()

    renew(0, scale)

    def sweep(i):
        collect(i % 2)
        renew(i % 2, lambda c: None)

    each(ITERS, sweep)
    collect(ITERS % 2)
    each(chunks, lambda c: weigh(ITERS % 2, c), 0)

    def deliver(k):
        for d in range(nx):
            s, q = source(k, d), pl.ds(k * nx + d, 1)
            weight_out[pl.ds(s, 1), :] = weights[q, :]
            holder_out[pl.ds(s, 1), :] = holders[q, :]
            used_out[pl.ds(s, 1), :] = req[s, 6:7, :]
            for half in range(2):
                row_out[pl.ds(2 * s + half, 1), :] = req[s, half : half + 1, :]

    each(nz, deliver, 0)
    theta_out[...] = theta[...]
    for copy in keeps:
        copy.wait()


def stats_kernel(
    docs, rows_ref, used_ref, holder_ref, theta_ref, weight_ref, gamma_ref, high_hbm, low_hbm, gamma_out, out_hbm,
    terms, high_ref, low_ref, sem, *sums,
):
    loads = [
        pltpu.make_async_copy(high_hbm, high_ref, sem.at[0]),
        pltpu.make_async_copy(low_hbm, low_ref, sem.at[1]),
    ]
    for copy in loads:
        copy.start()
    gamma_out[...] = gamma_ref[...]
    owners = holder_ref.shape[0]
    words, cols = out_hbm.shape

    def clear(i, _):
        for total in sums:
            total[pl.ds(pl.multiple_of(i * CAP, CAP), CAP), :] = jnp.zeros((CAP, cols), F32)
        return 0

    lax.fori_loop(0, words // CAP, clear, 0)
    for copy in loads:
        copy.wait()

    def term(s):
        weight = jnp.where(iota((docs, CAP), 0) == holder_ref[pl.ds(s, 1), :], weight_ref[pl.ds(s, 1), :], 0.0)
        whigh, wlow = halves(weight)
        thigh, tlow = halves(theta_ref[pl.ds(pl.multiple_of(s * docs, docs), docs), :])
        at = pl.ds(pl.multiple_of(s * CAP, CAP), CAP)
        share = dot(
            jnp.concatenate([whigh, whigh, wlow], axis=0), jnp.concatenate([thigh, tlow, thigh], axis=0), TN
        )
        terms[at, :] = share * (high_ref[at, :].astype(F32) + low_ref[at, :].astype(F32))

    def four(i, _):
        for u in range(4):
            term(i * 4 + u)
        return 0

    lax.fori_loop(0, owners // 4, four, 0)
    group = 16

    def one(s, _):
        def add(j, _):
            base = pl.multiple_of(s * CAP + j * group, group)
            now = terms.at[pl.ds(base, group), :]
            rows = [rows_ref[base + u] for u in range(group)]
            for start in range(0, group, len(sums)):
                news = []
                for k, total in enumerate(sums):
                    u = start + k
                    news.append(total[pl.ds(rows[u], 1), :] + now[u : u + 1, :])
                for k, total in enumerate(sums):
                    total[pl.ds(rows[start + k], 1), :] = news[k]
            return 0

        lax.fori_loop(0, (used_ref[s, 0] + group - 1) // group, add, 0)
        return 0

    lax.fori_loop(0, owners, one, 0)

    def finish(i, _):
        at = pl.ds(pl.multiple_of(i * CAP, CAP), CAP)
        sums[0][at, :] = functools.reduce(jnp.add, [total[at, :] for total in sums])
        pltpu.make_async_copy(sums[0].at[at], out_hbm.at[at], sem.at[2]).start()
        return 0

    lax.fori_loop(0, words // CAP, finish, 0)
    pltpu.make_async_copy(sums[0], out_hbm, sem.at[2]).wait()


VM = pl.BlockSpec(memory_space=pltpu.VMEM)
SM = pl.BlockSpec(memory_space=pltpu.SMEM)
AN = pl.BlockSpec(memory_space=pl.ANY)


def call(kernel, outs, in_specs, out_specs, scratch, **params):
    return pl.pallas_call(
        kernel,
        out_shape=outs,
        in_specs=in_specs,
        out_specs=out_specs,
        scratch_shapes=list(scratch),
        compiler_params=pltpu.CompilerParams(vmem_limit_bytes=60 * 2**20, **params),
    )


def shape(s, t=F32):
    return jax.ShapeDtypeStruct(s, t)


def per_device(log_beta, gamma_init, topic_prior, word_block, word_row, counts):
    docs, length = counts.shape
    words, cols = log_beta.shape
    owners, groups = lax.axis_size("docs"), lax.axis_size("topics")
    nz = grid_of(owners)
    nx = owners // nz
    slots = owners * CAP
    D, V = pltpu.SemaphoreType.DMA, pltpu.VMEM
    block = (docs, cols)
    gamma, theta, weight, holder, rows, used, high, low = call(
        functools.partial(main_kernel, nx, nz, groups),
        [
            shape(block), shape((owners * docs, cols)), shape((owners, CAP)), shape((owners, CAP), I32),
            shape((2 * owners, 128), I32), shape((owners, 128), I32),
            shape((slots, cols), BF), shape((slots, cols), BF),
        ],
        [VM] * 5 + [AN],
        [VM] * 6 + [AN] * 2,
        [
            V((owners, 8, 128), I32),
            V((owners, 8, 128), I32),
            pltpu.SMEM((owners, 2, 128), I32),
            V((words, cols), BF),
            V((words, 1, cols), F32),
            V((CAP, cols), F32),
            V((slots, cols), BF),
            V((slots, cols), BF),
            V((owners * docs, cols), F32),
            V(block, F32),
            V((groups, owners, CAP), F32),
            V((groups, owners, CAP), F32),
            V((2, groups, owners, CAP), F32),
            V((owners, CAP), F32),
            V((owners, CAP), I32),
            V((owners, CAP), F32),
            V((owners * docs, cols), F32),
            V((nx, nz, *block), F32),
            V((nz, *block), F32),
            V((nz, *block), F32),
            D((2,)), D((owners,)), D((owners,)), D((groups, nz // 2)), D((groups, nz // 2)),
            D((groups, nz // 2)), D((2, groups, nz // 2)),
            D((nz,)), D((nz,)), D((nx, nz)), D((nx, nz)), D((nx, nz)), D((nx, nz)), D((nz,)), D((nz,)),
        ],
        collective_id=1,
        has_side_effects=True,
    )(jnp.swapaxes(word_block, 1, 2), word_row, counts, gamma_init, topic_prior[None, :], log_beta)
    return call(
        functools.partial(stats_kernel, docs),
        [shape(block), shape((words, cols))],
        [SM, SM] + [VM] * 4 + [AN] * 2,
        [VM, AN],
        [V((slots, cols), F32), V((slots, cols), BF), V((slots, cols), BF), D((3,))]
        + [V((words, cols), F32)] * 4,
    )(rows.reshape(slots), used, holder, theta, weight, gamma, high, low)


def solution(mesh):
    return jax.shard_map(
        per_device,
        mesh=mesh,
        in_specs=(
            P("docs", "topics"),
            P("docs", "topics"),
            P("topics"),
            P("docs", None, None),
            P("docs", None),
            P("docs", None),
        ),
        out_specs=(P("docs", "topics"), P("docs", "topics")),
        check_vma=False,
    )
```

```python
import functools

import jax
import jax.numpy as jnp
from jax import lax
from jax.experimental import pallas as pl
from jax.experimental.pallas import tpu as pltpu
from jax.sharding import PartitionSpec as P

ITERS = 3
LIFT = 30.0
BF, F32, I32 = jnp.bfloat16, jnp.float32, jnp.int32
NN = (((1,), (0,)), ((), ()))
NT = (((1,), (1,)), ((), ()))
TN = (((0,), (0,)), ((), ()))
MESH = pl.DeviceIdType.MESH
CAP = 256


def dot(a, b, dims=NN):
    return lax.dot_general(a, b, dims, preferred_element_type=F32)


def halves(x):
    high = x.astype(BF)
    return high, (x - high.astype(F32)).astype(BF)


def iota(shape, dim):
    return lax.broadcasted_iota(I32, shape, dim)


def grid_of(owners):
    return {32: 8}.get(owners, owners // 2)


def pack(words, block_ref, row_ref, count_ref, out_ref):
    docs, length = row_ref.shape
    owners = out_ref.shape[0]
    earlier = (iota((length, length), 0) < iota((length, length), 1)).astype(BF)

    def step(d, carry):
        total, offset = carry
        owner, row, count = block_ref[d], row_ref[pl.ds(d, 1), :], count_ref[pl.ds(d, 1), :]
        owner = jnp.where(count > 0, owner, -1)
        member = (iota((owners, length), 0) == owner).astype(F32)
        before = dot(member.astype(BF), earlier) + offset
        rank = jnp.sum(member * before, axis=0, keepdims=True).astype(I32)
        place = (iota((CAP, length), 0) == rank).astype(BF)
        values = jnp.concatenate(
            [
                member * (row % 128).astype(F32),
                member * (row // 128).astype(F32),
                member * (count * docs + d).astype(F32),
            ],
            axis=0,
        ).astype(BF)
        total = total + dot(values, place, NT)
        return total, offset + jnp.sum(member, axis=1, keepdims=True)

    together = 4 if docs % 4 == 0 else 1

    def steps(i, carry):
        for u in range(together):
            carry = step(i * together + u, carry)
        return carry

    total, offset = lax.fori_loop(
        0, docs // together, steps, (jnp.zeros((3 * owners, CAP), F32), jnp.zeros((owners, 1), F32))
    )
    row = (total[owners : 2 * owners] * 128 + total[:owners]).astype(I32)
    row = jnp.minimum(jnp.maximum(row, 0), words - 1)
    rest = total[2 * owners :].astype(I32)
    used = jnp.broadcast_to(offset, (owners, 128)).astype(I32)
    for half in range(2):
        lanes = slice(half * 128, half * 128 + 128)
        out_ref[:, half, :] = row[:, lanes]
        out_ref[:, 2 + half, :] = rest[:, lanes] % docs
        out_ref[:, 4 + half, :] = rest[:, lanes] // docs
        out_ref[:, 6 + half, :] = used


def exp_digamma(g):
    z = g + 6.0
    total = 1.0 / g
    for i in range(1, 6):
        total = total + 1.0 / (g + float(i))
    inverse = 1.0 / z
    square = inverse * inverse
    series = square * (1 / 12 - square * (1 / 120 - square * (1 / 252 - square * (1 / 240))))
    return jnp.exp(jnp.log(z) - 0.5 * inverse - series - total)


def main_kernel(
    nx, nz, groups,
    block_ref, row_ref, count_ref, gamma_ref, prior_ref, beta_hbm,
    gamma_out, theta_out, weight_out, holder_out, row_out, used_out, high_hbm, low_hbm,
    request, req, rows, beta, wide, raw, high_ref, low_ref, theta, own_theta,
    shifts, scales, masses, counts, holders, weights, parts, xparts, zbase, zparts,
    local_sem, row_sem, rq_send, rq_recv, shift_send, shift_recv, mass_send, mass_recv,
    tz_send, tz_recv, tx_send, tx_recv, sx_send, sx_recv, sz_send, sz_recv,
):
    owners = nx * nz
    docs = gamma_ref.shape[0]
    me, top = lax.axis_index("docs"), lax.axis_index("topics")
    x, z = me // nz, me % nz
    chunks = half = nz // 2
    size = 2 * nx

    def at_x(d):
        return (x + d) % nx

    def at_z(d):
        return (z + d) % nz

    def block(i):
        return pl.ds(pl.multiple_of(i * docs, docs), docs)

    def slots(s):
        return pl.ds(pl.multiple_of(s * CAP, CAP), CAP)

    def lines(c):
        return pl.ds(pl.multiple_of(c * size, size), size)

    def remote(src, dst, send, recv, **device):
        return pltpu.make_async_remote_copy(
            src_ref=src, dst_ref=dst, send_sem=send, recv_sem=recv, device_id=device, device_id_type=MESH
        )

    def each(n, body, first=1):
        lax.fori_loop(first, n, lambda i, _: (body(i), 0)[1], 0)

    barrier = pltpu.get_barrier_semaphore()
    each(
        owners,
        lambda d: pl.semaphore_signal(
            barrier, inc=1, device_id={"docs": (me + d) % owners}, device_id_type=MESH
        ),
    )
    for d in range(1, groups):
        pl.semaphore_signal(barrier, inc=1, device_id={"topics": (top + d) % groups}, device_id_type=MESH)
    load = pltpu.make_async_copy(beta_hbm, beta, local_sem.at[0])
    load.start()
    pack(beta.shape[0], block_ref, row_ref, count_ref, request)
    first = exp_digamma(gamma_ref[...])
    own_theta[...] = first
    theta[block(me), :] = first
    req[me] = request[me]
    pl.semaphore_wait(barrier, owners - 1 + groups - 1)

    def turn(k):
        return jnp.where(k % 2 == 1, (k + 1) // 2, (nz - k // 2) % nz)

    def rq_copy(k, d):
        to, q = at_x(d) * nz + at_z(turn(k)), k * nx + d
        return remote(request.at[to], req.at[me], rq_send.at[q], rq_recv.at[q], docs=to)

    def others(action):
        for d in range(1, nx):
            action(0, d)

        def row(k):
            for d in range(nx):
                action(k, d)

        each(nz, row)

    def tz_copy(d):
        return remote(theta.at[block(me)], theta.at[block(me)], tz_send.at[d], tz_recv.at[d], docs=x * nz + at_z(d))

    def tx_copy(dx, dz):
        b = block(x * nz + at_z(nz - dz))
        return remote(theta.at[b], theta.at[b], tx_send.at[dx, dz], tx_recv.at[dx, dz], docs=at_x(dx) * nz + z)

    def far_copy(dx):
        b = block(me)
        to = at_x(dx) * nz + at_z(half)
        return remote(theta.at[b], theta.at[b], tx_send.at[dx, half], tx_recv.at[dx, half], docs=to)

    def sx_copy(dx, dz):
        b = block(at_x(dx) * nz + at_z(dz))
        to = at_x(dx) * nz + at_z(jnp.where(dz == half, half, 0))
        return remote(parts.at[b], xparts.at[dx, dz], sx_send.at[dx, dz], sx_recv.at[dx, dz], docs=to)

    def sz_copy(d):
        return remote(zbase.at[d], zparts.at[d], sz_send.at[d], sz_recv.at[d], docs=x * nz + at_z(d))

    def shift_copy(d, c):
        a = shifts.at[top, lines(c)]
        return remote(a, a, shift_send.at[d, c], shift_recv.at[d, c], topics=(top + d) % groups)

    def mass_copy(p, d, c):
        a = masses.at[p, top, lines(c)]
        return remote(a, a, mass_send.at[d, c], mass_recv.at[p, d, c], topics=(top + d) % groups)

    def source(k, d):
        return at_x(nx - d) * nz + at_z(nz - turn(k))

    def send_theta():
        each(nz, lambda d: tz_copy(d).start())
        for d in range(1, nx):
            tx_copy(d, 0).start()
        for d in range(1, nx):
            far_copy(d).start()

    def forward(k):
        dz = turn(k)
        tz_copy(dz).wait_recv()

        @pl.when(k < nz - 1)
        def _():
            for d in range(1, nx):
                tx_copy(d, dz).start()

    def forwards(c):
        each(jnp.minimum(2 * c + 4, nz), forward, 2 * c + 2)

    def mass_of(p, k, d):
        s, q = source(k, d), k * nx + d
        high, low = halves(theta[block(s), :])
        both = dot(jnp.concatenate([high, low], axis=0), high_ref[slots(s), :], NT)
        mass = both[:docs] + both[docs:] + dot(high, low_ref[slots(s), :], NT)
        mine = iota((docs, CAP), 0) == holders[pl.ds(q, 1), :]
        masses[p, top, pl.ds(q, 1), :] = jnp.sum(jnp.where(mine, mass, 0.0), axis=0, keepdims=True)

    def masses_of(p, c):
        def two(k):
            for d in range(1, nx):
                tx_copy(d, turn(k)).wait_recv()
            for d in range(nx):
                mass_of(p, k, d)

        each(2 * c + 2, two, 2 * c)
        each(groups, lambda d: mass_copy(p, d, c).start())

    def sent_theta():
        each(nz, lambda d: tz_copy(d).wait_send())

        def sent(k):
            for d in range(1, nx):
                tx_copy(d, k).wait_send()

        each(nz, sent, 0)

    others(lambda k, d: rq_copy(k, d).start())
    send_theta()
    load.wait()

    def widen(i):
        wide[slots(i), 0, :] = beta[slots(i), :].astype(F32)

    each(beta.shape[0] // CAP, widen, 0)

    def to_scalars(q):
        s = source(q // nx, q % nx)
        return pltpu.make_async_copy(req.at[s, 0:2, :], rows.at[s], row_sem.at[q])

    def arrive(q):
        @pl.when(q > 0)
        def _():
            rq_copy(q // nx, q % nx).wait_recv()

        to_scalars(q).start()
        s, at = source(q // nx, q % nx), pl.ds(q, 1)
        holders[at, :] = jnp.concatenate([req[s, 2:3, :], req[s, 3:4, :]], axis=1)
        counts[at, :] = jnp.concatenate([req[s, 4:5, :], req[s, 5:6, :]], axis=1).astype(F32)

    each(size, arrive, 0)
    each(2, forward)
    lead = (iota((8, 128), 1) == 0).astype(BF)

    def fetch(q):
        s = source(q // nx, q % nx)
        to_scalars(q).wait()
        for start in range(0, CAP, 16):
            values = [wide[rows[s, n // 128, n % 128]] for n in range(start, start + 16)]
            for u in range(16):
                raw[start + u : start + u + 1, :] = values[u]
        value = raw[...]
        peak = jnp.max(value, axis=1, keepdims=True)
        high, low = halves(jnp.exp(value - (peak - LIFT)))
        high_ref[slots(s), :] = high
        low_ref[slots(s), :] = low
        peaks = dot(lead, jnp.broadcast_to(peak, (CAP, 128)).astype(BF), NT)
        shifts[top, pl.ds(q, 1), :] = peaks[:1] - LIFT

    def begin(c):
        forwards(c)
        each(jnp.minimum(size * (c + 2), owners), arrive, size * (c + 1))
        each(size * (c + 1), fetch, size * c)
        each(groups, lambda d: shift_copy(d, c).start())
        masses_of(0, c)

    each(chunks, begin, 0)
    keeps = [
        pltpu.make_async_copy(high_ref, high_hbm, local_sem.at[0]),
        pltpu.make_async_copy(low_ref, low_hbm, local_sem.at[1]),
    ]
    for copy in keeps:
        copy.start()
    sent_theta()
    others(lambda k, d: rq_copy(k, d).wait_send())

    def scale(c):
        each(groups, lambda d: shift_copy(d, c).wait())
        peak = shifts[0, lines(c), :]
        for t in range(1, groups):
            peak = jnp.maximum(peak, shifts[t, lines(c), :])
        for t in range(groups):
            scales[t, lines(c), :] = jnp.exp(shifts[t, lines(c), :] - peak)

    def weigh(p, c):
        each(groups, lambda d: mass_copy(p, d, c).wait())
        norm = scales[0, lines(c), :] * masses[p, 0, lines(c), :]
        for t in range(1, groups):
            norm = norm + scales[t, lines(c), :] * masses[p, t, lines(c), :]
        weights[lines(c), :] = counts[lines(c), :] * scales[top, lines(c), :] / norm

    def part_of(k, d):
        s, q = source(k, d), k * nx + d
        mine = iota((docs, CAP), 0) == holders[pl.ds(q, 1), :]
        high, low = halves(jnp.where(mine, weights[pl.ds(q, 1), :], 0.0))
        both = dot(jnp.concatenate([high, low], axis=0), high_ref[slots(s), :])
        parts[block(s), :] = both[:docs] + both[docs:] + dot(high, low_ref[slots(s), :])

    def back(k):
        return (nz - turn(k)) % nz

    def parts_of(c):
        def two(k):
            for d in range(nx):
                part_of(k, d)
            for d in range(1, nx):
                sx_copy(d, back(k)).start()

        each(2 * c + 2, two, 2 * c)

        @pl.when(c == chunks - 1)
        def _():
            zbase[half] = parts[block(x * nz + at_z(half)), :]
            sz_copy(half).start()

    def joined(dz):
        total = parts[block(x * nz + at_z(dz)), :]
        for d in range(1, nx):
            sx_copy(d, dz).wait_recv()
            total = total + xparts[d, dz]
        return total

    def onward(k):
        zbase[back(k)] = joined(back(k))
        sz_copy(back(k)).start()

    def renew(p, prepare):
        def share(c):
            prepare(c)
            weigh(p, c)
            parts_of(c)

        each(chunks, share, 0)
        each(nz - 1, onward)
        total = joined(0)
        for d in range(1, nx):
            sx_copy(d, half).wait_recv()
            total = total + xparts[d, half]
        for d in range(1, nz):
            sz_copy(d).wait_recv()
            total = total + zparts[d]
        gamma = prior_ref[...] + own_theta[...] * total
        gamma_out[...] = gamma
        new = exp_digamma(gamma)
        own_theta[...] = new
        theta[block(me), :] = new
        send_theta()
        each(nz, lambda d: sz_copy(d).wait_send())

        def sent(k):
            for d in range(1, nx):
                sx_copy(d, k).wait_send()

        each(nz, sent, 0)

    def collect(p):
        each(2, forward)
        each(
            chunks,
            lambda c: (forwards(c), masses_of(p, c)),
            0,
        )
        sent_theta()

    renew(0, scale)

    def sweep(i):
        collect(i % 2)
        renew(i % 2, lambda c: None)

    each(ITERS, sweep)
    collect(ITERS % 2)
    each(chunks, lambda c: weigh(ITERS % 2, c), 0)

    def deliver(k):
        for d in range(nx):
            s, q = source(k, d), pl.ds(k * nx + d, 1)
            weight_out[pl.ds(s, 1), :] = weights[q, :]
            holder_out[pl.ds(s, 1), :] = holders[q, :]
            used_out[pl.ds(s, 1), :] = req[s, 6:7, :]
            for half in range(2):
                row_out[pl.ds(2 * s + half, 1), :] = req[s, half : half + 1, :]

    each(nz, deliver, 0)
    theta_out[...] = theta[...]
    for copy in keeps:
        copy.wait()


def stats_kernel(
    docs, rows_ref, used_ref, holder_ref, theta_ref, weight_ref, gamma_ref, high_hbm, low_hbm, gamma_out, out_hbm,
    terms, high_ref, low_ref, sem, *sums,
):
    loads = [
        pltpu.make_async_copy(high_hbm, high_ref, sem.at[0]),
        pltpu.make_async_copy(low_hbm, low_ref, sem.at[1]),
    ]
    for copy in loads:
        copy.start()
    gamma_out[...] = gamma_ref[...]
    owners = holder_ref.shape[0]
    words, cols = out_hbm.shape

    def clear(i, _):
        for total in sums:
            total[pl.ds(pl.multiple_of(i * CAP, CAP), CAP), :] = jnp.zeros((CAP, cols), F32)
        return 0

    lax.fori_loop(0, words // CAP, clear, 0)
    for copy in loads:
        copy.wait()

    def term(s):
        weight = jnp.where(iota((docs, CAP), 0) == holder_ref[pl.ds(s, 1), :], weight_ref[pl.ds(s, 1), :], 0.0)
        whigh, wlow = halves(weight)
        thigh, tlow = halves(theta_ref[pl.ds(pl.multiple_of(s * docs, docs), docs), :])
        at = pl.ds(pl.multiple_of(s * CAP, CAP), CAP)
        share = dot(
            jnp.concatenate([whigh, whigh, wlow], axis=0), jnp.concatenate([thigh, tlow, thigh], axis=0), TN
        )
        terms[at, :] = share * (high_ref[at, :].astype(F32) + low_ref[at, :].astype(F32))

    def four(i, _):
        for u in range(4):
            term(i * 4 + u)
        return 0

    lax.fori_loop(0, owners // 4, four, 0)
    group = 16

    def one(s, _):
        def add(j, _):
            base = pl.multiple_of(s * CAP + j * group, group)
            now = terms.at[pl.ds(base, group), :]
            rows = [rows_ref[base + u] for u in range(group)]
            for start in range(0, group, len(sums)):
                news = []
                for k, total in enumerate(sums):
                    u = start + k
                    news.append(total[pl.ds(rows[u], 1), :] + now[u : u + 1, :])
                for k, total in enumerate(sums):
                    total[pl.ds(rows[start + k], 1), :] = news[k]
            return 0

        lax.fori_loop(0, (used_ref[s, 0] + group - 1) // group, add, 0)
        return 0

    lax.fori_loop(0, owners, one, 0)

    def finish(i, _):
        at = pl.ds(pl.multiple_of(i * CAP, CAP), CAP)
        sums[0][at, :] = functools.reduce(jnp.add, [total[at, :] for total in sums])
        pltpu.make_async_copy(sums[0].at[at], out_hbm.at[at], sem.at[2]).start()
        return 0

    lax.fori_loop(0, words // CAP, finish, 0)
    pltpu.make_async_copy(sums[0], out_hbm, sem.at[2]).wait()


VM = pl.BlockSpec(memory_space=pltpu.VMEM)
SM = pl.BlockSpec(memory_space=pltpu.SMEM)
AN = pl.BlockSpec(memory_space=pl.ANY)


def call(kernel, outs, in_specs, out_specs, scratch, **params):
    return pl.pallas_call(
        kernel,
        out_shape=outs,
        in_specs=in_specs,
        out_specs=out_specs,
        scratch_shapes=list(scratch),
        compiler_params=pltpu.CompilerParams(vmem_limit_bytes=60 * 2**20, **params),
    )


def shape(s, t=F32):
    return jax.ShapeDtypeStruct(s, t)


def per_device(log_beta, gamma_init, topic_prior, word_block, word_row, counts):
    docs, length = counts.shape
    words, cols = log_beta.shape
    owners, groups = lax.axis_size("docs"), lax.axis_size("topics")
    nz = grid_of(owners)
    nx = owners // nz
    slots = owners * CAP
    D, V = pltpu.SemaphoreType.DMA, pltpu.VMEM
    block = (docs, cols)
    gamma, theta, weight, holder, rows, used, high, low = call(
        functools.partial(main_kernel, nx, nz, groups),
        [
            shape(block), shape((owners * docs, cols)), shape((owners, CAP)), shape((owners, CAP), I32),
            shape((2 * owners, 128), I32), shape((owners, 128), I32),
            shape((slots, cols), BF), shape((slots, cols), BF),
        ],
        [VM] * 5 + [AN],
        [VM] * 6 + [AN] * 2,
        [
            V((owners, 8, 128), I32),
            V((owners, 8, 128), I32),
            pltpu.SMEM((owners, 2, 128), I32),
            V((words, cols), BF),
            V((words, 1, cols), F32),
            V((CAP, cols), F32),
            V((slots, cols), BF),
            V((slots, cols), BF),
            V((owners * docs, cols), F32),
            V(block, F32),
            V((groups, owners, CAP), F32),
            V((groups, owners, CAP), F32),
            V((2, groups, owners, CAP), F32),
            V((owners, CAP), F32),
            V((owners, CAP), I32),
            V((owners, CAP), F32),
            V((owners * docs, cols), F32),
            V((nx, nz, *block), F32),
            V((nz, *block), F32),
            V((nz, *block), F32),
            D((2,)), D((owners,)), D((owners,)), D((owners,)), D((groups, nz // 2)), D((groups, nz // 2)),
            D((groups, nz // 2)), D((2, groups, nz // 2)),
            D((nz,)), D((nz,)), D((nx, nz)), D((nx, nz)), D((nx, nz)), D((nx, nz)), D((nz,)), D((nz,)),
        ],
        collective_id=1,
        has_side_effects=True,
    )(jnp.swapaxes(word_block, 1, 2), word_row, counts, gamma_init, topic_prior[None, :], log_beta)
    return call(
        functools.partial(stats_kernel, docs),
        [shape(block), shape((words, cols))],
        [SM, SM] + [VM] * 4 + [AN] * 2,
        [VM, AN],
        [V((slots, cols), F32), V((slots, cols), BF), V((slots, cols), BF), D((3,))]
        + [V((words, cols), F32)] * 4,
    )(rows.reshape(slots), used, holder, theta, weight, gamma, high, low)


def solution(mesh):
    return jax.shard_map(
        per_device,
        mesh=mesh,
        in_specs=(
            P("docs", "topics"),
            P("docs", "topics"),
            P("topics"),
            P("docs", None, None),
            P("docs", None),
            P("docs", None),
        ),
        out_specs=(P("docs", "topics"), P("docs", "topics")),
        check_vma=False,
    )
```

```python
import functools

import jax
import jax.numpy as jnp
from jax import lax
from jax.experimental import pallas as pl
from jax.experimental.pallas import tpu as pltpu
from jax.sharding import PartitionSpec as P

ITERS = 3
LIFT = 30.0
BF, F32, I32 = jnp.bfloat16, jnp.float32, jnp.int32
NN = (((1,), (0,)), ((), ()))
NT = (((1,), (1,)), ((), ()))
TN = (((0,), (0,)), ((), ()))
MESH = pl.DeviceIdType.MESH
CAP = 256


def dot(a, b, dims=NN):
    return lax.dot_general(a, b, dims, preferred_element_type=F32)


def halves(x):
    high = x.astype(BF)
    return high, (x - high.astype(F32)).astype(BF)


def iota(shape, dim):
    return lax.broadcasted_iota(I32, shape, dim)


def grid_of(owners):
    return {32: 8}.get(owners, owners // 2)


def pack(words, block_ref, row_ref, count_ref, out_ref):
    docs, length = row_ref.shape
    owners = out_ref.shape[0]
    earlier = (iota((length, length), 0) < iota((length, length), 1)).astype(BF)

    def step(d, carry):
        total, offset = carry
        owner, row, count = block_ref[d], row_ref[pl.ds(d, 1), :], count_ref[pl.ds(d, 1), :]
        owner = jnp.where(count > 0, owner, -1)
        member = (iota((owners, length), 0) == owner).astype(F32)
        before = dot(member.astype(BF), earlier) + offset
        rank = jnp.sum(member * before, axis=0, keepdims=True).astype(I32)
        place = (iota((CAP, length), 0) == rank).astype(BF)
        values = jnp.concatenate(
            [
                member * (row % 128).astype(F32),
                member * (row // 128).astype(F32),
                member * (count * docs + d).astype(F32),
            ],
            axis=0,
        ).astype(BF)
        total = total + dot(values, place, NT)
        return total, offset + jnp.sum(member, axis=1, keepdims=True)

    together = 4 if docs % 4 == 0 else 1

    def steps(i, carry):
        for u in range(together):
            carry = step(i * together + u, carry)
        return carry

    total, offset = lax.fori_loop(
        0, docs // together, steps, (jnp.zeros((3 * owners, CAP), F32), jnp.zeros((owners, 1), F32))
    )
    row = (total[owners : 2 * owners] * 128 + total[:owners]).astype(I32)
    row = jnp.minimum(jnp.maximum(row, 0), words - 1)
    row = (row // 8) * 16 + row % 8
    rest = total[2 * owners :].astype(I32)
    used = jnp.broadcast_to(offset, (owners, 128)).astype(I32)
    for half in range(2):
        lanes = slice(half * 128, half * 128 + 128)
        out_ref[:, half, :] = row[:, lanes]
        out_ref[:, 2 + half, :] = rest[:, lanes] % docs
        out_ref[:, 4 + half, :] = rest[:, lanes] // docs
        out_ref[:, 6 + half, :] = used


def exp_digamma(g):
    z = g + 6.0
    total = 1.0 / g
    for i in range(1, 6):
        total = total + 1.0 / (g + float(i))
    inverse = 1.0 / z
    square = inverse * inverse
    series = square * (1 / 12 - square * (1 / 120 - square * (1 / 252 - square * (1 / 240))))
    return jnp.exp(jnp.log(z) - 0.5 * inverse - series - total)


def main_kernel(
    nx, nz, groups,
    block_ref, row_ref, count_ref, gamma_ref, prior_ref, beta_hbm,
    gamma_out, theta_out, weight_out, holder_out, row_out, used_out, high_hbm, low_hbm,
    request, req, rows, beta, wide, raw_a, raw_b, high_ref, low_ref, theta, own_theta,
    shifts, scales, masses, counts, holders, weights, parts, xparts, zbase, zparts,
    local_sem, row_sem, rq_send, rq_recv, shift_send, shift_recv, mass_send, mass_recv,
    tz_send, tz_recv, tx_send, tx_recv, sx_send, sx_recv, sz_send, sz_recv,
):
    owners = nx * nz
    docs = gamma_ref.shape[0]
    me, top = lax.axis_index("docs"), lax.axis_index("topics")
    x, z = me // nz, me % nz
    chunks = nz // 2
    raws = (raw_a, raw_b)
    size = 2 * nx

    def at_x(d):
        return (x + d) % nx

    def at_z(d):
        return (z + d) % nz

    def block(i):
        return pl.ds(pl.multiple_of(i * docs, docs), docs)

    def slots(s):
        return pl.ds(pl.multiple_of(s * CAP, CAP), CAP)

    def lines(c):
        return pl.ds(pl.multiple_of(c * size, size), size)

    def remote(src, dst, send, recv, **device):
        return pltpu.make_async_remote_copy(
            src_ref=src, dst_ref=dst, send_sem=send, recv_sem=recv, device_id=device, device_id_type=MESH
        )

    def each(n, body, first=1):
        lax.fori_loop(first, n, lambda i, _: (body(i), 0)[1], 0)

    barrier = pltpu.get_barrier_semaphore()
    each(
        owners,
        lambda d: pl.semaphore_signal(
            barrier, inc=1, device_id={"docs": (me + d) % owners}, device_id_type=MESH
        ),
    )
    for d in range(1, groups):
        pl.semaphore_signal(barrier, inc=1, device_id={"topics": (top + d) % groups}, device_id_type=MESH)
    load = pltpu.make_async_copy(beta_hbm, beta, local_sem.at[0])
    load.start()
    pack(beta.shape[0], block_ref, row_ref, count_ref, request)
    first = exp_digamma(gamma_ref[...])
    own_theta[...] = first
    theta[block(me), :] = first
    req[me] = request[me]
    pl.semaphore_wait(barrier, owners - 1 + groups - 1)

    def turn(k):
        return jnp.where(k % 2 == 1, (k + 1) // 2, (nz - k // 2) % nz)

    def rq_copy(k, d):
        to, q = at_x(d) * nz + at_z(turn(k)), k * nx + d
        return remote(request.at[to], req.at[me], rq_send.at[q], rq_recv.at[q], docs=to)

    def others(action):
        for d in range(1, nx):
            action(0, d)

        def row(k):
            for d in range(nx):
                action(k, d)

        each(nz, row)

    def tz_copy(d):
        return remote(theta.at[block(me)], theta.at[block(me)], tz_send.at[d], tz_recv.at[d], docs=x * nz + at_z(d))

    def tx_copy(dx, dz):
        b = block(x * nz + at_z(nz - dz))
        return remote(theta.at[b], theta.at[b], tx_send.at[dx, dz], tx_recv.at[dx, dz], docs=at_x(dx) * nz + z)

    def sx_copy(dx, dz):
        b = block(at_x(dx) * nz + at_z(dz))
        return remote(parts.at[b], xparts.at[dx, dz], sx_send.at[dx, dz], sx_recv.at[dx, dz], docs=at_x(dx) * nz + z)

    def sz_copy(d):
        return remote(zbase.at[d], zparts.at[d], sz_send.at[d], sz_recv.at[d], docs=x * nz + at_z(d))

    def shift_copy(d, c):
        a = shifts.at[top, lines(c)]
        return remote(a, a, shift_send.at[d, c], shift_recv.at[d, c], topics=(top + d) % groups)

    def mass_copy(p, d, c):
        a = masses.at[p, top, lines(c)]
        return remote(a, a, mass_send.at[d, c], mass_recv.at[p, d, c], topics=(top + d) % groups)

    def source(k, d):
        return at_x(nx - d) * nz + at_z(nz - turn(k))

    def send_theta():
        each(nz, lambda d: tz_copy(d).start())
        for d in range(1, nx):
            tx_copy(d, 0).start()

    def forward(k):
        dz = turn(k)
        tz_copy(dz).wait_recv()
        for d in range(1, nx):
            tx_copy(d, dz).start()

    def forwards(c):
        each(jnp.minimum(2 * c + 4, nz), forward, 2 * c + 2)

    def mass_of(p, k, d):
        s, q = source(k, d), k * nx + d
        high, low = halves(theta[block(s), :])
        both = dot(jnp.concatenate([high, low], axis=0), high_ref[slots(s), :], NT)
        mass = both[:docs] + both[docs:] + dot(high, low_ref[slots(s), :], NT)
        mine = iota((docs, CAP), 0) == holders[pl.ds(q, 1), :]
        masses[p, top, pl.ds(q, 1), :] = jnp.sum(jnp.where(mine, mass, 0.0), axis=0, keepdims=True)

    def masses_of(p, c):
        for k in (2 * c, 2 * c + 1):
            for d in range(1, nx):
                tx_copy(d, turn(k)).wait_recv()
        for k in (2 * c, 2 * c + 1):
            for d in range(nx):
                mass_of(p, k, d)
        each(groups, lambda d: mass_copy(p, d, c).start())

    def sent_theta():
        each(nz, lambda d: tz_copy(d).wait_send())

        def sent(k):
            for d in range(1, nx):
                tx_copy(d, k).wait_send()

        each(nz, sent, 0)

    others(lambda k, d: rq_copy(k, d).start())
    send_theta()
    load.wait()

    def widen(i):
        value = beta[slots(i), :].astype(F32)
        for n in range(0, CAP, 8):
            for half in range(2):
                to = pl.ds(pl.multiple_of(i * 2 * CAP + 2 * n + 8 * half, 8), 8)
                wide[to, :] = value[n : n + 8, half * 128 : half * 128 + 128]

    each(beta.shape[0] // CAP, widen, 0)

    def to_scalars(q):
        s = source(q // nx, q % nx)
        return pltpu.make_async_copy(req.at[s, 0:2, :], rows.at[s], row_sem.at[q])

    def arrive(q):
        @pl.when(q > 0)
        def _():
            rq_copy(q // nx, q % nx).wait_recv()

        to_scalars(q).start()
        s, at = source(q // nx, q % nx), pl.ds(q, 1)
        holders[at, :] = jnp.concatenate([req[s, 2:3, :], req[s, 3:4, :]], axis=1)
        counts[at, :] = jnp.concatenate([req[s, 4:5, :], req[s, 5:6, :]], axis=1).astype(F32)

    each(size, arrive, 0)
    each(2, forward)
    lead = (iota((8, 128), 1) == 0).astype(BF)

    def fetch(i):
        pair = (2 * i, 2 * i + 1)
        homes = [source(q // nx, q % nx) for q in pair]
        for q in pair:
            to_scalars(q).wait()
        for s, raw in zip(homes, raws):
            for start in range(0, CAP, 16):
                values = [
                    wide[pl.ds(rows[s, n // 128, n % 128], 2, stride=8), :] for n in range(start, start + 16)
                ]
                for u in range(16):
                    raw[pl.ds(2 * start + u // 8 * 16 + u % 8, 2, stride=8), :] = values[u]
        for q, s, raw in zip(pair, homes, raws):
            sides = [
                jnp.concatenate([raw[n + 8 * half : n + 8 * half + 8, :] for n in range(0, 2 * CAP, 16)], axis=0)
                for half in range(2)
            ]
            peak = jnp.max(jnp.maximum(*sides), axis=1, keepdims=True)
            for half in range(2):
                high, low = halves(jnp.exp(sides[half] - (peak - LIFT)))
                high_ref[slots(s), half * 128 : half * 128 + 128] = high
                low_ref[slots(s), half * 128 : half * 128 + 128] = low
            peaks = dot(lead, jnp.broadcast_to(peak, (CAP, 128)).astype(BF), NT)
            shifts[top, pl.ds(q, 1), :] = peaks[:1] - LIFT

    def begin(c):
        forwards(c)
        each(jnp.minimum(size * (c + 2), owners), arrive, size * (c + 1))
        each(nx * (c + 1), fetch, nx * c)
        each(groups, lambda d: shift_copy(d, c).start())
        masses_of(0, c)

    each(chunks, begin, 0)
    keeps = [
        pltpu.make_async_copy(high_ref, high_hbm, local_sem.at[0]),
        pltpu.make_async_copy(low_ref, low_hbm, local_sem.at[1]),
    ]
    for copy in keeps:
        copy.start()
    sent_theta()
    others(lambda k, d: rq_copy(k, d).wait_send())

    def scale(c):
        each(groups, lambda d: shift_copy(d, c).wait())
        peak = shifts[0, lines(c), :]
        for t in range(1, groups):
            peak = jnp.maximum(peak, shifts[t, lines(c), :])
        for t in range(groups):
            scales[t, lines(c), :] = jnp.exp(shifts[t, lines(c), :] - peak)

    def weigh(p, c):
        each(groups, lambda d: mass_copy(p, d, c).wait())
        norm = scales[0, lines(c), :] * masses[p, 0, lines(c), :]
        for t in range(1, groups):
            norm = norm + scales[t, lines(c), :] * masses[p, t, lines(c), :]
        weights[lines(c), :] = counts[lines(c), :] * scales[top, lines(c), :] / norm

    def part_of(k, d):
        s, q = source(k, d), k * nx + d
        mine = iota((docs, CAP), 0) == holders[pl.ds(q, 1), :]
        high, low = halves(jnp.where(mine, weights[pl.ds(q, 1), :], 0.0))
        both = dot(jnp.concatenate([high, low], axis=0), high_ref[slots(s), :])
        parts[block(s), :] = both[:docs] + both[docs:] + dot(high, low_ref[slots(s), :])

    def back(k):
        return (nz - turn(k)) % nz

    def parts_of(c):
        for k in (2 * c, 2 * c + 1):
            for d in range(nx):
                part_of(k, d)
        for k in (2 * c, 2 * c + 1):
            for d in range(1, nx):
                sx_copy(d, back(k)).start()

    def joined(dz):
        total = parts[block(x * nz + at_z(dz)), :]
        for d in range(1, nx):
            sx_copy(d, dz).wait_recv()
            total = total + xparts[d, dz]
        return total

    def onward(k):
        zbase[back(k)] = joined(back(k))
        sz_copy(back(k)).start()

    def renew(p, prepare):
        def share(c):
            prepare(c)
            weigh(p, c)
            parts_of(c)

        each(chunks, share, 0)
        each(nz, onward)
        total = joined(0)
        for d in range(1, nz):
            sz_copy(d).wait_recv()
            total = total + zparts[d]
        gamma = prior_ref[...] + own_theta[...] * total
        gamma_out[...] = gamma
        new = exp_digamma(gamma)
        own_theta[...] = new
        theta[block(me), :] = new
        send_theta()
        each(nz, lambda d: sz_copy(d).wait_send())

        def sent(k):
            for d in range(1, nx):
                sx_copy(d, k).wait_send()

        each(nz, sent, 0)

    def collect(p):
        each(2, forward)
        each(
            chunks,
            lambda c: (forwards(c), masses_of(p, c)),
            0,
        )
        sent_theta()

    renew(0, scale)

    def sweep(i):
        collect(i % 2)
        renew(i % 2, lambda c: None)

    each(ITERS, sweep)
    collect(ITERS % 2)
    each(chunks, lambda c: weigh(ITERS % 2, c), 0)

    def deliver(k):
        for d in range(nx):
            s, q = source(k, d), pl.ds(k * nx + d, 1)
            weight_out[pl.ds(s, 1), :] = weights[q, :]
            holder_out[pl.ds(s, 1), :] = holders[q, :]
            used_out[pl.ds(s, 1), :] = req[s, 6:7, :]
            for half in range(2):
                row_out[pl.ds(2 * s + half, 1), :] = req[s, half : half + 1, :]

    each(nz, deliver, 0)
    theta_out[...] = theta[...]
    for copy in keeps:
        copy.wait()


def stats_kernel(
    docs, rows_ref, used_ref, holder_ref, theta_ref, weight_ref, gamma_ref, high_hbm, low_hbm, gamma_out, out_hbm,
    terms, high_ref, low_ref, sem, *sums,
):
    loads = [
        pltpu.make_async_copy(high_hbm, high_ref, sem.at[0]),
        pltpu.make_async_copy(low_hbm, low_ref, sem.at[1]),
    ]
    for copy in loads:
        copy.start()
    gamma_out[...] = gamma_ref[...]
    owners = holder_ref.shape[0]
    lines = out_hbm.shape[0]

    def clear(i, _):
        for total in sums:
            total[pl.ds(pl.multiple_of(i * CAP, CAP), CAP), :] = jnp.zeros((CAP, 128), F32)
        return 0

    lax.fori_loop(0, lines // CAP, clear, 0)
    for copy in loads:
        copy.wait()

    def term(s):
        weight = jnp.where(iota((docs, CAP), 0) == holder_ref[pl.ds(s, 1), :], weight_ref[pl.ds(s, 1), :], 0.0)
        whigh, wlow = halves(weight)
        thigh, tlow = halves(theta_ref[pl.ds(pl.multiple_of(s * docs, docs), docs), :])
        at = pl.ds(pl.multiple_of(s * CAP, CAP), CAP)
        share = dot(
            jnp.concatenate([whigh, whigh, wlow], axis=0), jnp.concatenate([thigh, tlow, thigh], axis=0), TN
        )
        term = share * (high_ref[at, :].astype(F32) + low_ref[at, :].astype(F32))
        for n in range(0, CAP, 8):
            for half in range(2):
                to = pl.ds(pl.multiple_of(s * 2 * CAP + 2 * n + 8 * half, 8), 8)
                terms[to, :] = term[n : n + 8, half * 128 : half * 128 + 128]

    def four(i, _):
        for u in range(4):
            term(i * 4 + u)
        return 0

    lax.fori_loop(0, owners // 4, four, 0)
    group = 16

    def one(s, _):
        def add(j, _):
            base = pl.multiple_of(s * CAP + j * group, group)
            now = terms.at[pl.ds(pl.multiple_of(2 * base, 2 * group), 2 * group), :]
            rows = [rows_ref[base + u] for u in range(group)]
            for start in range(0, group, len(sums)):
                news = []
                for k, total in enumerate(sums):
                    u = start + k
                    news.append(total[pl.ds(rows[u], 2, stride=8), :] + now[pl.ds(u // 8 * 16 + u % 8, 2, stride=8), :])
                for k, total in enumerate(sums):
                    total[pl.ds(rows[start + k], 2, stride=8), :] = news[k]
            return 0

        lax.fori_loop(0, (used_ref[s, 0] + group - 1) // group, add, 0)
        return 0

    lax.fori_loop(0, owners, one, 0)

    def finish(i, _):
        at = pl.ds(pl.multiple_of(i * CAP, CAP), CAP)
        sums[0][at, :] = functools.reduce(jnp.add, [total[at, :] for total in sums])
        pltpu.make_async_copy(sums[0].at[at], out_hbm.at[at], sem.at[2]).start()
        return 0

    lax.fori_loop(0, lines // CAP, finish, 0)
    pltpu.make_async_copy(sums[0], out_hbm, sem.at[2]).wait()


VM = pl.BlockSpec(memory_space=pltpu.VMEM)
SM = pl.BlockSpec(memory_space=pltpu.SMEM)
AN = pl.BlockSpec(memory_space=pl.ANY)


def call(kernel, outs, in_specs, out_specs, scratch, **params):
    return pl.pallas_call(
        kernel,
        out_shape=outs,
        in_specs=in_specs,
        out_specs=out_specs,
        scratch_shapes=list(scratch),
        compiler_params=pltpu.CompilerParams(vmem_limit_bytes=60 * 2**20, **params),
    )


def shape(s, t=F32):
    return jax.ShapeDtypeStruct(s, t)


def per_device(log_beta, gamma_init, topic_prior, word_block, word_row, counts):
    docs, length = counts.shape
    words, cols = log_beta.shape
    owners, groups = lax.axis_size("docs"), lax.axis_size("topics")
    nz = grid_of(owners)
    nx = owners // nz
    slots = owners * CAP
    D, V = pltpu.SemaphoreType.DMA, pltpu.VMEM
    block = (docs, cols)
    gamma, theta, weight, holder, rows, used, high, low = call(
        functools.partial(main_kernel, nx, nz, groups),
        [
            shape(block), shape((owners * docs, cols)), shape((owners, CAP)), shape((owners, CAP), I32),
            shape((2 * owners, 128), I32), shape((owners, 128), I32),
            shape((slots, cols), BF), shape((slots, cols), BF),
        ],
        [VM] * 5 + [AN],
        [VM] * 6 + [AN] * 2,
        [
            V((owners, 8, 128), I32),
            V((owners, 8, 128), I32),
            pltpu.SMEM((owners, 2, 128), I32),
            V((words, cols), BF),
            V((2 * words, 128), F32),
            V((2 * CAP, 128), F32),
            V((2 * CAP, 128), F32),
            V((slots, cols), BF),
            V((slots, cols), BF),
            V((owners * docs, cols), F32),
            V(block, F32),
            V((groups, owners, CAP), F32),
            V((groups, owners, CAP), F32),
            V((2, groups, owners, CAP), F32),
            V((owners, CAP), F32),
            V((owners, CAP), I32),
            V((owners, CAP), F32),
            V((owners * docs, cols), F32),
            V((nx, nz, *block), F32),
            V((nz, *block), F32),
            V((nz, *block), F32),
            D((2,)), D((owners,)), D((owners,)), D((owners,)), D((groups, nz // 2)), D((groups, nz // 2)),
            D((groups, nz // 2)), D((2, groups, nz // 2)),
            D((nz,)), D((nz,)), D((nx, nz)), D((nx, nz)), D((nx, nz)), D((nx, nz)), D((nz,)), D((nz,)),
        ],
        collective_id=1,
        has_side_effects=True,
    )(jnp.swapaxes(word_block, 1, 2), word_row, counts, gamma_init, topic_prior[None, :], log_beta)
    gamma, stats = call(
        functools.partial(stats_kernel, docs),
        [shape(block), shape((2 * words, 128))],
        [SM, SM] + [VM] * 4 + [AN] * 2,
        [VM, AN],
        [V((2 * slots, 128), F32), V((slots, cols), BF), V((slots, cols), BF), D((3,))]
        + [V((2 * words, 128), F32)] * 4,
    )(rows.reshape(slots), used, holder, theta, weight, gamma, high, low)
    return gamma, stats.reshape(words // 8, 2, 8, 128).swapaxes(1, 2).reshape(words, cols)


def solution(mesh):
    return jax.shard_map(
        per_device,
        mesh=mesh,
        in_specs=(
            P("docs", "topics"),
            P("docs", "topics"),
            P("topics"),
            P("docs", None, None),
            P("docs", None),
            P("docs", None),
        ),
        out_specs=(P("docs", "topics"), P("docs", "topics")),
        check_vma=False,
    )
```

```python
import functools

import jax
import jax.numpy as jnp
from jax import lax
from jax.experimental import pallas as pl
from jax.experimental.pallas import tpu as pltpu
from jax.sharding import PartitionSpec as P

ITERS = 3
LIFT = 30.0
BF, F32, I32 = jnp.bfloat16, jnp.float32, jnp.int32
NN = (((1,), (0,)), ((), ()))
NT = (((1,), (1,)), ((), ()))
TN = (((0,), (0,)), ((), ()))
MESH = pl.DeviceIdType.MESH
CAP = 256


def dot(a, b, dims=NN):
    return lax.dot_general(a, b, dims, preferred_element_type=F32)


def halves(x):
    high = x.astype(BF)
    return high, (x - high.astype(F32)).astype(BF)


def iota(shape, dim):
    return lax.broadcasted_iota(I32, shape, dim)


def grid_of(owners):
    return {32: 8}.get(owners, owners // 2)


def pack(words, block_ref, row_ref, count_ref, out_ref):
    docs, length = row_ref.shape
    owners = out_ref.shape[0]
    earlier = (iota((length, length), 0) < iota((length, length), 1)).astype(BF)

    def step(d, carry):
        total, offset = carry
        owner, row, count = block_ref[d], row_ref[pl.ds(d, 1), :], count_ref[pl.ds(d, 1), :]
        owner = jnp.where(count > 0, owner, -1)
        member = (iota((owners, length), 0) == owner).astype(F32)
        before = dot(member.astype(BF), earlier) + offset
        rank = jnp.sum(member * before, axis=0, keepdims=True).astype(I32)
        place = (iota((CAP, length), 0) == rank).astype(BF)
        values = jnp.concatenate(
            [
                member * (row % 128).astype(F32),
                member * (row // 128).astype(F32),
                member * (count * docs + d).astype(F32),
            ],
            axis=0,
        ).astype(BF)
        total = total + dot(values, place, NT)
        return total, offset + jnp.sum(member, axis=1, keepdims=True)

    together = 4 if docs % 4 == 0 else 1

    def steps(i, carry):
        for u in range(together):
            carry = step(i * together + u, carry)
        return carry

    total, offset = lax.fori_loop(
        0, docs // together, steps, (jnp.zeros((3 * owners, CAP), F32), jnp.zeros((owners, 1), F32))
    )
    row = (total[owners : 2 * owners] * 128 + total[:owners]).astype(I32)
    row = jnp.minimum(jnp.maximum(row, 0), words - 1)
    row = (row // 8) * 16 + row % 8
    rest = total[2 * owners :].astype(I32)
    used = jnp.broadcast_to(offset, (owners, 128)).astype(I32)
    for half in range(2):
        lanes = slice(half * 128, half * 128 + 128)
        out_ref[:, half, :] = row[:, lanes]
        out_ref[:, 2 + half, :] = rest[:, lanes] % docs
        out_ref[:, 4 + half, :] = rest[:, lanes] // docs
        out_ref[:, 6 + half, :] = used


def exp_digamma(g):
    z = g + 6.0
    total = 1.0 / g
    for i in range(1, 6):
        total = total + 1.0 / (g + float(i))
    inverse = 1.0 / z
    square = inverse * inverse
    series = square * (1 / 12 - square * (1 / 120 - square * (1 / 252 - square * (1 / 240))))
    return jnp.exp(jnp.log(z) - 0.5 * inverse - series - total)


def main_kernel(
    nx, nz, groups,
    block_ref, row_ref, count_ref, gamma_ref, prior_ref, beta_hbm,
    gamma_out, theta_hbm, weight_out, holder_out, row_out, used_out, high_hbm, low_hbm,
    request, req, rows, beta, wide, raw_a, raw_b, high_ref, low_ref, theta, own_theta,
    shifts, scales, masses, counts, holders, weights, parts, xparts, zbase, zparts,
    local_sem, row_sem, rq_send, rq_recv, shift_send, shift_recv, mass_send, mass_recv,
    tz_send, tz_recv, tx_send, tx_recv, sx_send, sx_recv, sz_send, sz_recv,
):
    owners = nx * nz
    docs = gamma_ref.shape[0]
    me, top = lax.axis_index("docs"), lax.axis_index("topics")
    x, z = me // nz, me % nz
    chunks = nz // 2
    spread = sorted(range(1, nx), key=lambda d: abs(2 * d - nx))
    raws = (raw_a, raw_b)
    size = 2 * nx

    def at_x(d):
        return (x + d) % nx

    def at_z(d):
        return (z + d) % nz

    def block(i):
        return pl.ds(pl.multiple_of(i * docs, docs), docs)

    def slots(s):
        return pl.ds(pl.multiple_of(s * CAP, CAP), CAP)

    def lines(c):
        return pl.ds(pl.multiple_of(c * size, size), size)

    def remote(src, dst, send, recv, **device):
        return pltpu.make_async_remote_copy(
            src_ref=src, dst_ref=dst, send_sem=send, recv_sem=recv, device_id=device, device_id_type=MESH
        )

    def each(n, body, first=1):
        lax.fori_loop(first, n, lambda i, _: (body(i), 0)[1], 0)

    barrier = pltpu.get_barrier_semaphore()
    each(
        owners,
        lambda d: pl.semaphore_signal(
            barrier, inc=1, device_id={"docs": (me + d) % owners}, device_id_type=MESH
        ),
    )
    for d in range(1, groups):
        pl.semaphore_signal(barrier, inc=1, device_id={"topics": (top + d) % groups}, device_id_type=MESH)
    load = pltpu.make_async_copy(beta_hbm, beta, local_sem.at[0])
    load.start()
    pack(beta.shape[0], block_ref, row_ref, count_ref, request)
    first = exp_digamma(gamma_ref[...])
    own_theta[...] = first
    theta[block(me), :] = first
    req[me] = request[me]
    pl.semaphore_wait(barrier, owners - 1 + groups - 1)

    def turn(k):
        return jnp.where(k % 2 == 1, (k + 1) // 2, (nz - k // 2) % nz)

    def rq_copy(k, d):
        to, q = at_x(d) * nz + at_z(turn(k)), k * nx + d
        return remote(request.at[to], req.at[me], rq_send.at[q], rq_recv.at[q], docs=to)

    def others(action):
        for d in range(1, nx):
            action(0, d)

        def row(k):
            for d in range(nx):
                action(k, d)

        each(nz, row)

    def tz_copy(d):
        return remote(theta.at[block(me)], theta.at[block(me)], tz_send.at[d], tz_recv.at[d], docs=x * nz + at_z(d))

    def tx_copy(dx, dz):
        b = block(x * nz + at_z(nz - dz))
        return remote(theta.at[b], theta.at[b], tx_send.at[dx, dz], tx_recv.at[dx, dz], docs=at_x(dx) * nz + z)

    def sx_copy(dx, dz):
        b = block(at_x(dx) * nz + at_z(dz))
        return remote(parts.at[b], xparts.at[dx, dz], sx_send.at[dx, dz], sx_recv.at[dx, dz], docs=at_x(dx) * nz + z)

    def sz_copy(d):
        return remote(zbase.at[d], zparts.at[d], sz_send.at[d], sz_recv.at[d], docs=x * nz + at_z(d))

    def shift_copy(d, c):
        a = shifts.at[top, lines(c)]
        return remote(a, a, shift_send.at[d, c], shift_recv.at[d, c], topics=(top + d) % groups)

    def mass_copy(p, d, c):
        a = masses.at[p, top, lines(c)]
        return remote(a, a, mass_send.at[d, c], mass_recv.at[p, d, c], topics=(top + d) % groups)

    def source(k, d):
        return at_x(nx - d) * nz + at_z(nz - turn(k))

    def send_theta():
        for d in range(1, nx):
            tx_copy(d, 0).start()
        for k in range(1, nz):
            tz_copy((k + 1) // 2 if k % 2 else nz - k // 2).start()

    def forward(k):
        dz = turn(k)
        tz_copy(dz).wait_recv()
        for d in spread:
            tx_copy(d, dz).start()

    def forwards(c):
        each(jnp.minimum(2 * c + 4, nz), forward, 2 * c + 2)

    def mass_of(p, k, d):
        s, q = source(k, d), k * nx + d
        high, low = halves(theta[block(s), :])
        both = dot(jnp.concatenate([high, low], axis=0), high_ref[slots(s), :], NT)
        mass = both[:docs] + both[docs:] + dot(high, low_ref[slots(s), :], NT)
        mine = iota((docs, CAP), 0) == holders[pl.ds(q, 1), :]
        masses[p, top, pl.ds(q, 1), :] = jnp.sum(jnp.where(mine, mass, 0.0), axis=0, keepdims=True)

    def masses_of(p, c):
        for k in (2 * c, 2 * c + 1):
            for d in range(1, nx):
                tx_copy(d, turn(k)).wait_recv()
        for k in (2 * c, 2 * c + 1):
            for d in range(nx):
                mass_of(p, k, d)
        for d in range(1, groups):
            mass_copy(p, d, c).start()

    def sent_theta():
        each(nz, lambda d: tz_copy(d).wait_send())

        def sent(k):
            for d in range(1, nx):
                tx_copy(d, k).wait_send()

        each(nz, sent, 0)

    others(lambda k, d: rq_copy(k, d).start())
    send_theta()
    load.wait()

    def widen(i):
        value = beta[slots(i), :].astype(F32)
        for n in range(0, CAP, 8):
            for half in range(2):
                to = pl.ds(pl.multiple_of(i * 2 * CAP + 2 * n + 8 * half, 8), 8)
                wide[to, :] = value[n : n + 8, half * 128 : half * 128 + 128]

    each(beta.shape[0] // CAP, widen, 0)

    def to_scalars(q):
        s = source(q // nx, q % nx)
        return pltpu.make_async_copy(req.at[s, 0:2, :], rows.at[s], row_sem.at[q])

    def arrive(q):
        @pl.when(q > 0)
        def _():
            rq_copy(q // nx, q % nx).wait_recv()

        to_scalars(q).start()
        s, at = source(q // nx, q % nx), pl.ds(q, 1)
        holders[at, :] = jnp.concatenate([req[s, 2:3, :], req[s, 3:4, :]], axis=1)
        counts[at, :] = jnp.concatenate([req[s, 4:5, :], req[s, 5:6, :]], axis=1).astype(F32)

    each(size, arrive, 0)
    each(2, forward)
    lead = (iota((8, 128), 1) == 0).astype(BF)

    def fetch(i):
        pair = (2 * i, 2 * i + 1)
        homes = [source(q // nx, q % nx) for q in pair]
        for q in pair:
            to_scalars(q).wait()
        for s, raw in zip(homes, raws):
            for start in range(0, CAP, 16):
                values = [
                    wide[pl.ds(rows[s, n // 128, n % 128], 2, stride=8), :] for n in range(start, start + 16)
                ]
                for u in range(16):
                    raw[pl.ds(2 * start + u // 8 * 16 + u % 8, 2, stride=8), :] = values[u]
        for q, s, raw in zip(pair, homes, raws):
            sides = [
                jnp.concatenate([raw[n + 8 * half : n + 8 * half + 8, :] for n in range(0, 2 * CAP, 16)], axis=0)
                for half in range(2)
            ]
            peak = jnp.max(jnp.maximum(*sides), axis=1, keepdims=True)
            for half in range(2):
                high, low = halves(jnp.exp(sides[half] - (peak - LIFT)))
                high_ref[slots(s), half * 128 : half * 128 + 128] = high
                low_ref[slots(s), half * 128 : half * 128 + 128] = low
            peaks = dot(lead, jnp.broadcast_to(peak, (CAP, 128)).astype(BF), NT)
            shifts[top, pl.ds(q, 1), :] = peaks[:1] - LIFT

    def begin(c):
        forwards(c)
        each(jnp.minimum(size * (c + 2), owners), arrive, size * (c + 1))
        each(nx * (c + 1), fetch, nx * c)
        each(groups, lambda d: shift_copy(d, c).start())
        masses_of(0, c)

    each(chunks, begin, 0)
    keeps = [
        pltpu.make_async_copy(high_ref, high_hbm, local_sem.at[0]),
        pltpu.make_async_copy(low_ref, low_hbm, local_sem.at[1]),
    ]
    for copy in keeps:
        copy.start()
    sent_theta()
    others(lambda k, d: rq_copy(k, d).wait_send())

    def scale(c):
        each(groups, lambda d: shift_copy(d, c).wait())
        peak = shifts[0, lines(c), :]
        for t in range(1, groups):
            peak = jnp.maximum(peak, shifts[t, lines(c), :])
        for t in range(groups):
            scales[t, lines(c), :] = jnp.exp(shifts[t, lines(c), :] - peak)

    def weigh(p, c):
        for d in range(1, groups):
            mass_copy(p, d, c).wait()
        norm = scales[0, lines(c), :] * masses[p, 0, lines(c), :]
        for t in range(1, groups):
            norm = norm + scales[t, lines(c), :] * masses[p, t, lines(c), :]
        weights[lines(c), :] = counts[lines(c), :] * scales[top, lines(c), :] / norm

    def part_of(k, d):
        s, q = source(k, d), k * nx + d
        mine = iota((docs, CAP), 0) == holders[pl.ds(q, 1), :]
        high, low = halves(jnp.where(mine, weights[pl.ds(q, 1), :], 0.0))
        both = dot(jnp.concatenate([high, low], axis=0), high_ref[slots(s), :])
        parts[block(s), :] = both[:docs] + both[docs:] + dot(high, low_ref[slots(s), :])

    def back(k):
        return (nz - turn(k)) % nz

    def parts_of(c):
        for k in (2 * c, 2 * c + 1):
            for d in range(nx):
                part_of(k, d)
        for k in (2 * c, 2 * c + 1):
            for d in spread:
                sx_copy(d, back(k)).start()

    def joined(dz):
        total = parts[block(x * nz + at_z(dz)), :]
        for d in range(1, nx):
            sx_copy(d, dz).wait_recv()
            total = total + xparts[d, dz]
        return total

    def onward(k):
        zbase[back(k)] = joined(back(k))
        sz_copy(back(k)).start()

    def renew(p, prepare):
        def share(c):
            prepare(c)
            weigh(p, c)
            parts_of(c)

        each(chunks, share, 0)
        each(nz, onward)
        total = joined(0)
        for d in range(1, nz):
            sz_copy(d).wait_recv()
            total = total + zparts[d]
        gamma = prior_ref[...] + own_theta[...] * total
        gamma_out[...] = gamma
        new = exp_digamma(gamma)
        own_theta[...] = new
        theta[block(me), :] = new
        send_theta()
        each(nz, lambda d: sz_copy(d).wait_send())

        def sent(k):
            for d in range(1, nx):
                sx_copy(d, k).wait_send()

        each(nz, sent, 0)

    def collect(p):
        each(nz, forward)
        each(chunks, lambda c: masses_of(p, c), 0)
        sent_theta()

    renew(0, scale)

    def sweep(i):
        collect(i % 2)
        renew(i % 2, lambda c: None)

    each(ITERS, sweep)
    collect(ITERS % 2)
    keep = pltpu.make_async_copy(theta, theta_hbm, local_sem.at[2])
    keep.start()

    def deliver(k):
        for d in range(nx):
            s, q = source(k, d), pl.ds(k * nx + d, 1)
            holder_out[pl.ds(s, 1), :] = holders[q, :]
            used_out[pl.ds(s, 1), :] = req[s, 6:7, :]
            for half in range(2):
                row_out[pl.ds(2 * s + half, 1), :] = req[s, half : half + 1, :]

    each(nz, deliver, 0)
    each(chunks, lambda c: weigh(ITERS % 2, c), 0)

    def hand_out(k):
        for d in range(nx):
            weight_out[pl.ds(source(k, d), 1), :] = weights[pl.ds(k * nx + d, 1), :]

    each(nz, hand_out, 0)
    for copy in (*keeps, keep):
        copy.wait()


def stats_kernel(
    docs, rows_ref, used_ref, holder_ref, weight_ref, gamma_ref, theta_hbm, high_hbm, low_hbm, gamma_out, out_hbm,
    terms, theta_ref, high_ref, low_ref, sem, *sums,
):
    loads = [
        pltpu.make_async_copy(high_hbm, high_ref, sem.at[0]),
        pltpu.make_async_copy(low_hbm, low_ref, sem.at[1]),
        pltpu.make_async_copy(theta_hbm, theta_ref, sem.at[3]),
    ]
    for copy in loads:
        copy.start()
    gamma_out[...] = gamma_ref[...]
    owners = holder_ref.shape[0]
    lines = out_hbm.shape[0]

    def clear(i, _):
        for total in sums:
            total[pl.ds(pl.multiple_of(i * CAP, CAP), CAP), :] = jnp.zeros((CAP, 128), F32)
        return 0

    lax.fori_loop(0, lines // CAP, clear, 0)
    for copy in loads:
        copy.wait()

    def term(s):
        weight = jnp.where(iota((docs, CAP), 0) == holder_ref[pl.ds(s, 1), :], weight_ref[pl.ds(s, 1), :], 0.0)
        whigh, wlow = halves(weight)
        thigh, tlow = halves(theta_ref[pl.ds(pl.multiple_of(s * docs, docs), docs), :])
        at = pl.ds(pl.multiple_of(s * CAP, CAP), CAP)
        share = dot(
            jnp.concatenate([whigh, whigh, wlow], axis=0), jnp.concatenate([thigh, tlow, thigh], axis=0), TN
        )
        term = share * (high_ref[at, :].astype(F32) + low_ref[at, :].astype(F32))
        for n in range(0, CAP, 8):
            for half in range(2):
                to = pl.ds(pl.multiple_of(s * 2 * CAP + 2 * n + 8 * half, 8), 8)
                terms[to, :] = term[n : n + 8, half * 128 : half * 128 + 128]

    def four(i, _):
        for u in range(4):
            term(i * 4 + u)
        return 0

    lax.fori_loop(0, owners // 4, four, 0)
    group = 16

    def one(s, _):
        def add(j, _):
            base = pl.multiple_of(s * CAP + j * group, group)
            now = terms.at[pl.ds(pl.multiple_of(2 * base, 2 * group), 2 * group), :]
            rows = [rows_ref[base + u] for u in range(group)]
            for start in range(0, group, len(sums)):
                news = []
                for k, total in enumerate(sums):
                    u = start + k
                    news.append(total[pl.ds(rows[u], 2, stride=8), :] + now[pl.ds(u // 8 * 16 + u % 8, 2, stride=8), :])
                for k, total in enumerate(sums):
                    total[pl.ds(rows[start + k], 2, stride=8), :] = news[k]
            return 0

        lax.fori_loop(0, (used_ref[s, 0] + group - 1) // group, add, 0)
        return 0

    lax.fori_loop(0, owners, one, 0)

    def finish(i, _):
        at = pl.ds(pl.multiple_of(i * CAP, CAP), CAP)
        sums[0][at, :] = functools.reduce(jnp.add, [total[at, :] for total in sums])
        pltpu.make_async_copy(sums[0].at[at], out_hbm.at[at], sem.at[2]).start()
        return 0

    lax.fori_loop(0, lines // CAP, finish, 0)
    pltpu.make_async_copy(sums[0], out_hbm, sem.at[2]).wait()


VM = pl.BlockSpec(memory_space=pltpu.VMEM)
SM = pl.BlockSpec(memory_space=pltpu.SMEM)
AN = pl.BlockSpec(memory_space=pl.ANY)


def call(kernel, outs, in_specs, out_specs, scratch, **params):
    return pl.pallas_call(
        kernel,
        out_shape=outs,
        in_specs=in_specs,
        out_specs=out_specs,
        scratch_shapes=list(scratch),
        compiler_params=pltpu.CompilerParams(vmem_limit_bytes=60 * 2**20, **params),
    )


def shape(s, t=F32):
    return jax.ShapeDtypeStruct(s, t)


def per_device(log_beta, gamma_init, topic_prior, word_block, word_row, counts):
    docs, length = counts.shape
    words, cols = log_beta.shape
    owners, groups = lax.axis_size("docs"), lax.axis_size("topics")
    nz = grid_of(owners)
    nx = owners // nz
    slots = owners * CAP
    D, V = pltpu.SemaphoreType.DMA, pltpu.VMEM
    block = (docs, cols)
    gamma, theta, weight, holder, rows, used, high, low = call(
        functools.partial(main_kernel, nx, nz, groups),
        [
            shape(block), shape((owners * docs, cols)), shape((owners, CAP)), shape((owners, CAP), I32),
            shape((2 * owners, 128), I32), shape((owners, 128), I32),
            shape((slots, cols), BF), shape((slots, cols), BF),
        ],
        [VM] * 5 + [AN],
        [VM, AN] + [VM] * 4 + [AN] * 2,
        [
            V((owners, 8, 128), I32),
            V((owners, 8, 128), I32),
            pltpu.SMEM((owners, 2, 128), I32),
            V((words, cols), BF),
            V((2 * words, 128), F32),
            V((2 * CAP, 128), F32),
            V((2 * CAP, 128), F32),
            V((slots, cols), BF),
            V((slots, cols), BF),
            V((owners * docs, cols), F32),
            V(block, F32),
            V((groups, owners, CAP), F32),
            V((groups, owners, CAP), F32),
            V((2, groups, owners, CAP), F32),
            V((owners, CAP), F32),
            V((owners, CAP), I32),
            V((owners, CAP), F32),
            V((owners * docs, cols), F32),
            V((nx, nz, *block), F32),
            V((nz, *block), F32),
            V((nz, *block), F32),
            D((3,)), D((owners,)), D((owners,)), D((owners,)), D((groups, nz // 2)), D((groups, nz // 2)),
            D((groups, nz // 2)), D((2, groups, nz // 2)),
            D((nz,)), D((nz,)), D((nx, nz)), D((nx, nz)), D((nx, nz)), D((nx, nz)), D((nz,)), D((nz,)),
        ],
        collective_id=1,
        has_side_effects=True,
    )(jnp.swapaxes(word_block, 1, 2), word_row, counts, gamma_init, topic_prior[None, :], log_beta)
    gamma, stats = call(
        functools.partial(stats_kernel, docs),
        [shape(block), shape((2 * words, 128))],
        [SM, SM] + [VM] * 3 + [AN] * 3,
        [VM, AN],
        [V((2 * slots, 128), F32), V((owners * docs, cols), F32), V((slots, cols), BF), V((slots, cols), BF), D((4,))]
        + [V((2 * words, 128), F32)] * 4,
    )(rows.reshape(slots), used, holder, weight, gamma, theta, high, low)
    return gamma, stats.reshape(words // 8, 2, 8, 128).swapaxes(1, 2).reshape(words, cols)


def solution(mesh):
    return jax.shard_map(
        per_device,
        mesh=mesh,
        in_specs=(
            P("docs", "topics"),
            P("docs", "topics"),
            P("topics"),
            P("docs", None, None),
            P("docs", None),
            P("docs", None),
        ),
        out_specs=(P("docs", "topics"), P("docs", "topics")),
        check_vma=False,
    )
```
